512 devices in a mesh: tm: 4 (over z_hi), mem: 4 (over y), tile: 32 (over x, z_lo, core).
Axes of the slice: x: 4, y: 4, z: 16 (z_hi: 4, z_lo: 4; z = z_hi * 4 + z_lo), core: 2. Of those that a mesh axis runs over, the one named last changes fastest.
Arguments:
- control: float32 [40, 2, 128, 256], P('mem', None, 'tile'), may hold values from -6 to 6
- vertical_modes: float32 [64, 2], replicated, may hold values from -4 to 4
- mode_counts: int32 [128], P('tile'), may hold values from 1 to 2, as said below
- perturbations: bfloat16 [40, 8, 64, 128, 256], P('mem', 'tm', None, 'tile'), may hold values from -6 to 6
- slot_index: int32 [12], P('tm'), may hold values from 0 to 7, as said below
- blend_weight: float32 [12], P('tm'), may hold values from 0 to 1
Outputs:
- increment: float32 [12, 64, 128, 256], P('tm', None, 'tile')
The draws below stay inside these ranges and needn't reach their ends.
Inputs may be any that keep to these rules, and one draw needn't show every extreme that they name: slot_index[w] // 2 == w // 3. `mode_counts`: both ends of the range occur.
All inputs are finite; a program needn't handle non-finite values.
Results may differ from the reference program's by a relative error of at most 0.0003.
Values sent between devices are 32-bit elements; how exact they have to be, the bound alone decides.
A program may use at most 64 MiB of HBM per device.

```python
import math
import jax
import jax.numpy as jnp
from jax import lax

LEV = 64
VM = 2
SMOOTH = 4
SLOT_DEV = 2
WIN_DEV = 3
GY = 256
ENS = 40
SLOTS = 8
WIN = 12
NX = 128


def draw_slot_index(key, part):
    blocks = jnp.arange(WIN) // WIN_DEV
    offsets = jax.random.randint(key, (WIN,), 0, SLOT_DEV)
    return (blocks * SLOT_DEV + offsets).astype(jnp.int32)


def draw_mode_counts(key, part):
    first_key = jax.random.fold_in(key, 11)
    second_key = jax.random.fold_in(key, 23)
    counts = jax.random.randint(first_key, (NX,), 1, VM + 1)
    where = jax.random.randint(second_key, (), 0, NX)
    counts = counts.at[where].set(1)
    counts = counts.at[(where + 1) % NX].set(VM)
    return counts.astype(jnp.int32)


def block_scale(stream_key, dims, pieces, smallest, largest):
    gain, own = 1.0, jax.random.fold_in(stream_key, 6)
    for position, parts in pieces:
        steps = jnp.exp(jax.random.uniform(jax.random.fold_in(own, position), (parts,), jnp.float32, smallest / len(pieces), largest / len(pieces)))
        gain = gain * jnp.repeat(steps, dims[position] // parts).reshape([-1 if axis == position else 1 for axis in range(len(dims))])
    return gain


def bell_draw(rng, shape, scale, bound, pieces=(), held_as=jnp.bfloat16):
    array = scale * jax.random.normal(rng, shape, jnp.float32)
    if pieces:
        array = array * block_scale(rng, shape, pieces, -0.22, 0.18)
    return jnp.clip(array, -bound, bound).astype(held_as)


def setup_inputs(seed: int = 0) -> dict:
    splits = jax.random.split(jax.random.key(seed), 7)
    control = bell_draw(splits[0], (ENS, VM, NX, GY), 1.0, 6.0, ((0, 4), (2, 32)), jnp.float32)
    vertical_modes = bell_draw(splits[1], (LEV, VM), 1.0, 4.0, (), jnp.float32)
    mode_counts = draw_mode_counts(jax.random.fold_in(splits[6], 71), 0)
    perturbations = bell_draw(splits[3], (ENS, SLOTS, LEV, NX, GY), 1.0, 6.0, ((0, 4), (1, 4), (3, 32)))
    slot_index = draw_slot_index(jax.random.fold_in(splits[6], 71), 0)
    blend_weight = jnp.clip(1.0 * jax.random.uniform(splits[5], (WIN,), jnp.float32) ** block_scale(splits[5], (WIN,), ((0, 4),), -0.2, 0.2), 0.0, 1.0)
    return dict(control=control, vertical_modes=vertical_modes, mode_counts=mode_counts, perturbations=perturbations, slot_index=slot_index, blend_weight=blend_weight)


diffusion = 0.24

def relax_global(field):
    neighbours = jnp.roll(field, -1, axis=2) + jnp.roll(field, 1, axis=2)
    padded = jnp.pad(field, ((0, 0), (0, 0), (0, 0), (1, 1)))
    lateral = padded[:, :, :, 2:] + padded[:, :, :, :-2]
    return field + diffusion * (neighbours + lateral - 4.0 * field)

def reference(control, vertical_modes, mode_counts, perturbations, slot_index, blend_weight):
    smoothed = control
    for repeat in range(SMOOTH):
        smoothed = relax_global(smoothed)
    localized = jnp.zeros((ENS, LEV, NX, GY), jnp.float32)
    for mode_index in range(VM):
        keep_mode = (mode_index < mode_counts).astype(jnp.float32)
        masked = keep_mode[None, :, None] * smoothed[:, mode_index]
        localized = localized + vertical_modes[:, mode_index][None, :, None, None] * masked[:, None]
    norm_factor = 1.0 / math.sqrt(ENS - 1)
    slots = []
    for slot in range(SLOTS):
        member_total = lax.optimization_barrier(jnp.sum(localized * perturbations[:, slot].astype(jnp.float32), axis=0))
        slots.append(member_total * norm_factor)
    slot_increment = jnp.stack(slots)
    cumulative = jnp.cumsum(slot_increment, axis=0)
    previous = jnp.concatenate([jnp.zeros((1, LEV, NX, GY), jnp.float32), cumulative[:-1]], axis=0)
    weight = blend_weight[:, None, None, None]
    return weight * cumulative[slot_index] + (1.0 - weight) * previous[slot_index]
```

```python
import functools
import math

import jax
import jax.numpy as jnp
from jax import lax
from jax.experimental import pallas as pl
from jax.experimental.pallas import tpu as pltpu
from jax.sharding import PartitionSpec as P

SMOOTH = 4
DIFFUSION = 0.24
CHUNKS = 4
MESH = pl.DeviceIdType.MESH


def smooth_group(halo, f_ref, counts, norm, group, rows):
    lane = lax.broadcasted_iota(jnp.int32, (rows, 128), 1)
    first, last = lane == 0, lane == 127
    base = group * 64

    def load(x, h):
        tile, inner = (x + 4) // 4, x % 4
        return halo[tile, pl.ds(base + h * 4 + inner, rows, 8), :]

    field = {(x, h): load(x, h) for x in range(-4, 8) for h in range(2)}
    for step in range(SMOOTH):
        lo, hi = -3 + step, 7 - step
        new = {}
        for x in range(lo, hi):
            pair = [field[x, 0], field[x, 1]]
            up = [pltpu.roll(v, 1, 1) for v in pair]
            down = [pltpu.roll(v, 127, 1) for v in pair]
            lateral = [
                jnp.where(first, 0.0, up[0]) + jnp.where(last, down[1], down[0]),
                jnp.where(first, up[0], up[1]) + jnp.where(last, 0.0, down[1]),
            ]
            for h in range(2):
                near = field[x - 1, h] + field[x + 1, h]
                new[x, h] = (1.0 - 4.0 * DIFFUSION) * pair[h] + DIFFUSION * (
                    near + lateral[h]
                )
        field = new
    mode = lax.broadcasted_iota(jnp.int32, (rows, 128), 0) % 2
    for x in range(4):
        scales = [jnp.where(m < counts[x], norm, 0.0) for m in range(2)]
        scale = jnp.where(mode == 0, scales[0], scales[1])
        for h in range(2):
            f_ref[pl.ds(base + h * 4 + x, rows, 8), :] = field[x, h] * scale


def kernel(
    n_tm, n_mem, n_tile, members, windows,
    ctrl, pert_hbm, modes, counts, slot_index, weight,
    out,
    halo, pert, f_ref, far, near_r, near_l, mail_a, mail_b, mail_r, mail_l,
    za_out, za_in, zb_in, gath,
    load_sems, halo_send, halo_recv, send, recv,
):
    t, m = lax.axis_index("tm"), lax.axis_index("mem")
    tile = lax.axis_index("tile")
    nc = far.shape[0]
    lc = far.shape[2]
    pairs = lc // 2
    quarter_pairs = nc * pairs
    norm = 1.0 / math.sqrt(members * n_mem - 1)

    ctrl_load = pltpu.make_async_copy(ctrl, halo.at[1], load_sems.at[0])
    ctrl_load.start()
    pert_load = pltpu.make_async_copy(pert_hbm, pert, load_sems.at[1])
    pert_load.start()

    tile_r, tile_l = lax.rem(tile + 1, n_tile), lax.rem(tile + n_tile - 1, n_tile)
    mem_r, mem_l = lax.rem(m + 1, n_mem), lax.rem(m + n_mem - 1, n_mem)
    mem_f = lax.rem(m + 2, n_mem)
    tm_r, tm_l = lax.rem(t + 1, n_tm), lax.rem(t + n_tm - 1, n_tm)
    barrier = pltpu.get_barrier_semaphore()
    partners = (
        {"tile": tile_r}, {"tile": tile_l}, {"mem": mem_r}, {"mem": mem_l},
        {"mem": mem_f}, {"tm": tm_r}, {"tm": tm_l},
    )
    for partner in partners:
        pl.semaphore_signal(barrier, inc=1, device_id=partner, device_id_type=MESH)
    ctrl_load.wait()
    pl.semaphore_wait(barrier, len(partners))

    def remote(src, dst, s, r, device):
        return pltpu.make_async_remote_copy(
            src_ref=src, dst_ref=dst, send_sem=s, recv_sem=r,
            device_id=device, device_id_type=MESH,
        )

    to_right = remote(halo.at[1], halo.at[0], halo_send.at[0], halo_recv.at[0], {"tile": tile_r})
    to_left = remote(halo.at[1], halo.at[2], halo_send.at[1], halo_recv.at[1], {"tile": tile_l})
    to_right.start()
    to_left.start()
    to_right.wait()
    to_left.wait()

    fields = 2 * members
    for group in range(0, fields, 8):
        smooth_group(halo, f_ref, counts, norm, group // 8, min(8, fields - group))
    pert_load.wait()

    def part(quarter, chunk, store):
        def body(p, carry):
            lp = quarter * quarter_pairs + chunk * pairs + p
            v = [[modes[mode, 2 * lp + j] for mode in range(2)] for j in range(2)]
            acc = [[None, None], [None, None]]
            for k in range(members):
                f0 = f_ref[pl.ds(16 * k, 8), :]
                f1 = f_ref[pl.ds(16 * k + 8, 8), :]
                loc = [v[j][0] * f0 + v[j][1] * f1 for j in range(2)]
                for s in range(2):
                    x = pert[k, s, lp].astype(jnp.float32)
                    for j in range(2):
                        term = loc[j] * x[8 * j : 8 * j + 8]
                        acc[s][j] = term if k == 0 else acc[s][j] + term
            for s in range(2):
                for j in range(2):
                    store(s, 2 * p + j, acc[s][j])
            return carry

        lax.fori_loop(0, pairs, body, 0)

    def into(ref):
        def store(s, level, value):
            ref[s, level] = value
        return store

    def channel(k, chunk, src, dst, device):
        return remote(src, dst, send.at[k, chunk], recv.at[k, chunk], device)

    right, left = {"mem": mem_r}, {"mem": mem_l}
    across = {"mem": mem_f}
    onward = {"tm": tm_r}
    back = {"tm": tm_l}

    far_r = [channel(0, c, far.at[c, 0], mail_a.at[c], right) for c in range(nc)]
    far_l = [channel(1, c, far.at[c, 1], mail_b.at[c], left) for c in range(nc)]
    sum_r = [channel(2, c, near_r.at[c], mail_r.at[c], right) for c in range(nc)]
    sum_l = [channel(3, c, near_l.at[c], mail_l.at[c], left) for c in range(nc)]
    chain = [channel(4, c, za_out.at[c], za_in.at[c], onward) for c in range(nc)]
    around = [channel(5, c, za_out.at[c], zb_in.at[c], back) for c in range(nc)]
    relay = [channel(5, c, zb_in.at[c], zb_in.at[c], back) for c in range(nc)]
    slots_r = [channel(6, c, gath.at[m, c, pl.ds(0, 2)], gath.at[m, c, pl.ds(0, 2)], right) for c in range(nc)]
    slots_l = [channel(7, c, gath.at[m, c, pl.ds(0, 2)], gath.at[m, c, pl.ds(0, 2)], left) for c in range(nc)]
    pass_r = [channel(8, c, gath.at[mem_l, c, 0], gath.at[mem_l, c, 0], right) for c in range(nc)]
    pass_l = [channel(9, c, gath.at[mem_r, c, 1], gath.at[mem_r, c, 1], left) for c in range(nc)]
    early_r = [channel(10, c, gath.at[m, c, 2], gath.at[m, c, 2], right) for c in range(nc)]
    early_l = [channel(11, c, gath.at[m, c, 2], gath.at[m, c, 2], left) for c in range(nc)]
    early_f = [channel(12, c, gath.at[m, c, 2], gath.at[m, c, 2], across) for c in range(nc)]

    for c in range(nc):
        part(mem_f, c, into(far.at[c]))
        far_r[c].start()
        far_l[c].start()
    for c in range(nc):
        part(mem_r, c, into(near_r.at[c]))
        part(mem_l, c, into(near_l.at[c]))
    for c in range(nc):
        part(m, c, into(gath.at[m, c]))

    for c in range(nc):
        far_r[c].wait_recv()
        near_r[c, 0] += mail_a[c]
        sum_r[c].start()
        far_l[c].wait_recv()
        near_l[c, 1] += mail_b[c]
        sum_l[c].start()

    for c in range(nc):
        sum_r[c].wait_recv()
        sum_l[c].wait_recv()
        total = jnp.zeros_like(za_out[c])
        for s in range(2):
            value = gath[m, c, s] + (mail_r[c, s] + mail_l[c, s])
            gath[m, c, s] = value
            total = total + value
        za_out[c] = total

        @pl.when(t < 2)
        def _():
            chain[c].start()

        @pl.when(t == 0)
        def _():
            around[c].start()

        slots_r[c].start()
        slots_l[c].start()

    for c in range(nc):
        slots_r[c].wait_recv()
        pass_r[c].start()
        slots_l[c].wait_recv()
        pass_l[c].start()

    for c in range(nc):
        @pl.when(t == 2)
        def _():
            chain[c].wait_recv()
            za_out[c] += za_in[c]
            chain[c].start()

        @pl.when(t == 3)
        def _():
            around[c].wait_recv()
            relay[c].start()

    for c in range(nc):
        pass_r[c].wait_recv()
        pass_l[c].wait_recv()

    for c in range(nc):
        @pl.when(t == 0)
        def _():
            gath[m, c, 2] = jnp.zeros_like(gath[m, c, 2])

        @pl.when(t == 1)
        def _():
            chain[c].wait_recv()
            gath[m, c, 2] = za_in[c]

        @pl.when(t == 2)
        def _():
            relay[c].wait_recv()
            gath[m, c, 2] = za_in[c] + zb_in[c]

        @pl.when(t == 3)
        def _():
            chain[c].wait_recv()
            gath[m, c, 2] = za_in[c] + zb_in[c]

        early_r[c].start()
        early_l[c].start()
        early_f[c].start()

    scale = []
    for w in range(windows):
        b = weight[w]
        later = slot_index[w] - 2 * t == 1
        scale.append((jnp.where(later, 1.0, b), jnp.where(later, b, 0.0)))

    for c in range(nc):
        early_r[c].wait_recv()
        early_l[c].wait_recv()
        early_f[c].wait_recv()
        for q in range(n_mem):
            def body(level, carry):
                r0, r1, e = (gath[q, c, i, level] for i in range(3))
                for w in range(windows):
                    out[w, q * nc * lc + c * lc + level] = e + (scale[w][0] * r0 + scale[w][1] * r1)
                return carry
            lax.fori_loop(0, lc, body, 0)

    for group in (far_r, far_l, sum_r, sum_l, slots_r, slots_l, pass_r, pass_l, early_r, early_l, early_f):
        for copy in group:
            copy.wait_send()
    for c in range(nc):
        @pl.when(t < 3)
        def _():
            chain[c].wait_send()

        @pl.when(t == 0)
        def _():
            around[c].wait_send()

        @pl.when(t == 3)
        def _():
            relay[c].wait_send()


def solution(mesh):
    n_tm, n_mem, n_tile = (mesh.shape[a] for a in ("tm", "mem", "tile"))

    def folded(x):
        *lead, rows, columns = x.shape
        x = x.reshape(*lead, rows, columns // 128, 128)
        x = jnp.swapaxes(x, -3, -2)
        return x.reshape(*lead, rows * (columns // 128), 128)

    def per_device(control, vertical_modes, mode_counts, perturbations, slot_index, blend_weight):
        members, slots, levels = perturbations.shape[:3]
        windows = slot_index.shape[0]
        ctrl = folded(control).reshape(-1, 128)
        pert = folded(perturbations).reshape(members, slots, levels // 2, 16, 128)
        rows = ctrl.shape[0]
        nc = CHUNKS
        lc = levels // n_mem // nc
        f32 = jnp.float32
        slot = (nc, slots, lc, 8, 128)
        one = (nc, lc, 8, 128)
        smem = pl.BlockSpec(memory_space=pltpu.SMEM)
        hbm = pl.BlockSpec(memory_space=pl.ANY)
        dma = pltpu.SemaphoreType.DMA
        out = pl.pallas_call(
            functools.partial(kernel, n_tm, n_mem, n_tile, members, windows),
            out_shape=jax.ShapeDtypeStruct((windows, levels, 8, 128), f32),
            in_specs=[hbm, hbm, smem, smem, smem, smem],
            out_specs=pl.BlockSpec(memory_space=pltpu.VMEM),
            scratch_shapes=[
                pltpu.VMEM((3, rows, 128), f32),
                pltpu.VMEM(pert.shape, jnp.bfloat16),
                pltpu.VMEM((rows, 128), f32),
                pltpu.VMEM(slot, f32), pltpu.VMEM(slot, f32), pltpu.VMEM(slot, f32),
                pltpu.VMEM(one, f32), pltpu.VMEM(one, f32),
                pltpu.VMEM(slot, f32), pltpu.VMEM(slot, f32),
                pltpu.VMEM(one, f32), pltpu.VMEM(one, f32), pltpu.VMEM(one, f32),
                pltpu.VMEM((n_mem, nc, 3, lc, 8, 128), f32),
                dma((2,)), dma((2,)), dma((2,)), dma((13, nc)), dma((13, nc)),
            ],
            compiler_params=pltpu.CompilerParams(collective_id=0, has_side_effects=True),
        )(ctrl, pert, vertical_modes.T, mode_counts, slot_index, blend_weight)
        out = out.reshape(windows, levels, 2, 4, 128)
        return jnp.swapaxes(out, -3, -2).reshape(windows, levels, 4, 256)

    return jax.shard_map(
        per_device,
        mesh=mesh,
        in_specs=(
            P("mem", None, "tile", None), P(), P("tile"),
            P("mem", "tm", None, "tile", None), P("tm"), P("tm"),
        ),
        out_specs=P("tm", None, "tile", None),
        check_vma=False,
    )
```

```python
import functools
import math
from contextlib import nullcontext as scope

import jax
import jax.numpy as jnp
from jax import lax
from jax.experimental import pallas as pl
from jax.experimental.pallas import tpu as pltpu
from jax.sharding import PartitionSpec as P

SMOOTH = 4
DIFFUSION = 0.24
CHUNKS = 4
MESH = pl.DeviceIdType.MESH


def smooth_group(halo, f_ref, counts, norm, group, rows):
    lane = lax.broadcasted_iota(jnp.int32, (rows, 128), 1)
    first, last = lane == 0, lane == 127
    base = group * 64

    def load(x, h):
        tile, inner = (x + 4) // 4, x % 4
        return halo[tile, pl.ds(base + h * 4 + inner, rows, 8), :]

    field = {(x, h): load(x, h) for x in range(-4, 8) for h in range(2)}
    for step in range(SMOOTH):
        lo, hi = -3 + step, 7 - step
        new = {}
        for x in range(lo, hi):
            pair = [field[x, 0], field[x, 1]]
            up = [pltpu.roll(v, 1, 1) for v in pair]
            down = [pltpu.roll(v, 127, 1) for v in pair]
            lateral = [
                jnp.where(first, 0.0, up[0]) + jnp.where(last, down[1], down[0]),
                jnp.where(first, up[0], up[1]) + jnp.where(last, 0.0, down[1]),
            ]
            for h in range(2):
                near = field[x - 1, h] + field[x + 1, h]
                new[x, h] = (1.0 - 4.0 * DIFFUSION) * pair[h] + DIFFUSION * (
                    near + lateral[h]
                )
        field = new
    mode = lax.broadcasted_iota(jnp.int32, (rows, 128), 0) % 2
    for x in range(4):
        scales = [jnp.where(m < counts[x], norm, 0.0) for m in range(2)]
        scale = jnp.where(mode == 0, scales[0], scales[1])
        for h in range(2):
            f_ref[pl.ds(base + h * 4 + x, rows, 8), :] = field[x, h] * scale


def kernel(
    n_tm, n_mem, n_tile, members, windows,
    ctrl, pert_hbm, modes_hbm, counts_hbm, index_hbm, weight_hbm,
    gath, scale,
    halo, pert, f_ref, far, near_r, near_l, mail_a, mail_b, mail_r, mail_l,
    za_out, za_in, zb_in, modes, counts, slot_index, weight,
    load_sems, halo_send, halo_recv, send, recv, ready_next, ready_back,
):
    t, m = lax.axis_index("tm"), lax.axis_index("mem")
    tile = lax.axis_index("tile")
    nc = far.shape[0]
    lc = far.shape[2]
    pairs = lc // 2
    quarter_pairs = nc * pairs
    norm = 1.0 / math.sqrt(members * n_mem - 1)

    tile_r, tile_l = lax.rem(tile + 1, n_tile), lax.rem(tile + n_tile - 1, n_tile)
    mem_r, mem_l = lax.rem(m + 1, n_mem), lax.rem(m + n_mem - 1, n_mem)
    mem_f = lax.rem(m + 2, n_mem)
    tm_r, tm_l = lax.rem(t + 1, n_tm), lax.rem(t + n_tm - 1, n_tm)
    right, left, across = {"mem": mem_r}, {"mem": mem_l}, {"mem": mem_f}
    onward, back = {"tm": tm_r}, {"tm": tm_l}

    def signal(sem, device):
        pl.semaphore_signal(sem, inc=1, device_id=device, device_id_type=MESH)

    barrier = pltpu.get_barrier_semaphore()
    partners = ({"tile": tile_r}, {"tile": tile_l}, right, left, across)
    for partner in partners:
        signal(barrier, partner)

    @pl.when(t < 2)
    def _():
        signal(barrier, onward)

    @pl.when((t == 0) | (t == 3))
    def _():
        signal(barrier, back)

    loads = [
        pltpu.make_async_copy(src, dst, load_sems.at[k])
        for k, (src, dst) in enumerate((
            (ctrl, halo.at[1]), (counts_hbm, counts), (modes_hbm, modes),
            (index_hbm, slot_index), (weight_hbm, weight), (pert_hbm, pert),
        ))
    ]
    for load in loads:
        load.start()
    with scope("barrier"):
        loads[0].wait()
        extra = jnp.where(t == 0, 0, jnp.where(t == 2, 2, 1))
        pl.semaphore_wait(barrier, len(partners) + extra)

    def remote(src, dst, s, r, device):
        return pltpu.make_async_remote_copy(
            src_ref=src, dst_ref=dst, send_sem=s, recv_sem=r,
            device_id=device, device_id_type=MESH,
        )

    to_right = remote(halo.at[1], halo.at[0], halo_send.at[0], halo_recv.at[0], {"tile": tile_r})
    to_left = remote(halo.at[1], halo.at[2], halo_send.at[1], halo_recv.at[1], {"tile": tile_l})
    to_right.start()
    to_left.start()

    @pl.when((t == 1) | (t == 2))
    def _():
        signal(ready_next, back)

    @pl.when(t >= 2)
    def _():
        signal(ready_back, onward)

    for load in loads[1:5]:
        load.wait()
    for w in range(windows):
        b = weight[w]
        later = slot_index[w] - 2 * t == 1
        scale[w, 0] = jnp.full((8, 128), jnp.where(later, 1.0, b), jnp.float32)
        scale[w, 1] = jnp.full((8, 128), jnp.where(later, b, 0.0), jnp.float32)
    with scope("halo"):
        to_right.wait()
        to_left.wait()

    with scope("smooth"):
        fields = 2 * members
        for group in range(0, fields, 8):
            smooth_group(halo, f_ref, counts, norm, group // 8, min(8, fields - group))
        loads[5].wait()

    def part(quarter, chunk, dst):
        def body(p, carry):
            lp = quarter * quarter_pairs + chunk * pairs + p
            v = [[modes[mode, 2 * lp + j] for mode in range(2)] for j in range(2)]
            acc = [[None, None], [None, None]]
            for k in range(members):
                f0 = f_ref[pl.ds(16 * k, 8), :]
                f1 = f_ref[pl.ds(16 * k + 8, 8), :]
                loc = [v[j][0] * f0 + v[j][1] * f1 for j in range(2)]
                for s in range(2):
                    x = pert[k, s, lp].astype(jnp.float32)
                    for j in range(2):
                        term = loc[j] * x[8 * j : 8 * j + 8]
                        acc[s][j] = term if k == 0 else acc[s][j] + term
            for s in range(2):
                for j in range(2):
                    dst[s, 2 * p + j] = acc[s][j]
            return carry

        if pairs == 1:
            body(0, 0)
        else:
            lax.fori_loop(0, pairs, body, 0)

    def channel(k, chunk, src, dst, device):
        return remote(src, dst, send.at[k, chunk], recv.at[k, chunk], device)

    def both(ref):
        return ref.at[pl.ds(0, 2)]

    far_r = [channel(0, c, far.at[c, 0], mail_a.at[c], right) for c in range(nc)]
    far_l = [channel(1, c, far.at[c, 1], mail_b.at[c], left) for c in range(nc)]
    sum_r = [channel(2, c, near_r.at[c], mail_r.at[c], right) for c in range(nc)]
    sum_l = [channel(3, c, near_l.at[c], mail_l.at[c], left) for c in range(nc)]
    chain = [channel(4, c, za_out.at[c], za_in.at[c], onward) for c in range(nc)]
    around = [channel(5, c, za_out.at[c], zb_in.at[c], back) for c in range(nc)]
    relay = [channel(5, c, zb_in.at[c], zb_in.at[c], back) for c in range(nc)]
    slots_r = [channel(6, c, both(gath.at[m, c]), both(gath.at[m, c]), right) for c in range(nc)]
    slots_l = [channel(7, c, both(gath.at[m, c]), both(gath.at[m, c]), left) for c in range(nc)]
    pass_r = [channel(8, c, gath.at[mem_l, c, 0], gath.at[mem_l, c, 0], right) for c in range(nc)]
    pass_l = [channel(9, c, gath.at[mem_r, c, 1], gath.at[mem_r, c, 1], left) for c in range(nc)]
    early_r = [channel(10, c, gath.at[m, c, 2], gath.at[m, c, 2], right) for c in range(nc)]
    early_l = [channel(11, c, gath.at[m, c, 2], gath.at[m, c, 2], left) for c in range(nc)]
    early_f = [channel(12, c, gath.at[m, c, 2], gath.at[m, c, 2], across) for c in range(nc)]

    with scope("far"):
        for c in range(nc):
            part(mem_f, c, far.at[c])
            far_r[c].start()
            far_l[c].start()
    with scope("near"):
        for c in range(nc):
            part(mem_r, c, near_r.at[c])
            part(mem_l, c, near_l.at[c])
        for c in range(nc):
            part(m, c, gath.at[m, c])

    for c in range(nc):
        with scope(f"A{c}"):
            far_r[c].wait_recv()
            near_r[c, 0] += mail_a[c]
            sum_r[c].start()
            far_l[c].wait_recv()
            near_l[c, 1] += mail_b[c]
            sum_l[c].start()

    with scope("R"):
        @pl.when(t < 2)
        def _():
            pl.semaphore_wait(ready_next, 1)

        @pl.when((t == 0) | (t == 3))
        def _():
            pl.semaphore_wait(ready_back, 1)

    for c in range(nc):
        with scope(f"B{c}"):
            sum_r[c].wait_recv()
            sum_l[c].wait_recv()
            for level in range(lc):
                total = None
                for s in range(2):
                    value = gath[m, c, s, level] + (mail_r[c, s, level] + mail_l[c, s, level])
                    gath[m, c, s, level] = value
                    total = value if s == 0 else total + value
                za_out[c, level] = total

            @pl.when(t < 2)
            def _():
                chain[c].start()

            @pl.when(t == 0)
            def _():
                around[c].start()

            slots_r[c].start()
            slots_l[c].start()

    for c in range(nc):
        with scope(f"Z{c}"):
            @pl.when(t == 2)
            def _():
                chain[c].wait_recv()
                za_out[c] += za_in[c]
                chain[c].start()

            @pl.when(t == 3)
            def _():
                around[c].wait_recv()
                relay[c].start()
        with scope(f"D{c}"):
            slots_r[c].wait_recv()
            pass_r[c].start()
            slots_l[c].wait_recv()
            pass_l[c].start()

    for c in range(nc):
        with scope(f"E{c}"):
            @pl.when(t == 0)
            def _():
                gath[m, c, 2] = jnp.zeros_like(gath[m, c, 2])

            @pl.when(t == 1)
            def _():
                chain[c].wait_recv()
                gath[m, c, 2] = za_in[c]

            @pl.when(t == 2)
            def _():
                relay[c].wait_recv()
                gath[m, c, 2] = za_in[c] + zb_in[c]

            @pl.when(t == 3)
            def _():
                chain[c].wait_recv()
                gath[m, c, 2] = za_in[c] + zb_in[c]

            early_r[c].start()
            early_l[c].start()
            early_f[c].start()

    with scope("P"):
        for c in range(nc):
            pass_r[c].wait_recv()
            pass_l[c].wait_recv()

    for c in range(nc):
        with scope(f"H{c}"):
            early_r[c].wait_recv()
            early_l[c].wait_recv()
            early_f[c].wait_recv()

    for group in (far_r, far_l, sum_r, sum_l, slots_r, slots_l, pass_r, pass_l, early_r, early_l, early_f):
        for copy in group:
            copy.wait_send()
    for c in range(nc):
        @pl.when(t < 3)
        def _():
            chain[c].wait_send()

        @pl.when(t == 0)
        def _():
            around[c].wait_send()

        @pl.when(t == 3)
        def _():
            relay[c].wait_send()


def blend_kernel(gath, scale, out, block, sems):
    n_mem, nc, _, lc = gath.shape[:4]
    windows = block.shape[0]
    copies = []
    for w in range(windows):
        a, b = scale[w, 0], scale[w, 1]
        for q in range(n_mem):
            for c in range(nc):
                for level in range(lc):
                    r0, r1, e = (gath[q, c, i, level] for i in range(3))
                    block[w, (q * nc + c) * lc + level] = e + (a * r0 + b * r1)
        copies.append(pltpu.make_async_copy(block.at[w], out.at[w], sems.at[w]))
        copies[-1].start()
    for copy in copies:
        copy.wait()


def solution(mesh):
    n_tm, n_mem, n_tile = (mesh.shape[a] for a in ("tm", "mem", "tile"))

    def folded(x):
        *lead, rows, columns = x.shape
        x = x.reshape(*lead, rows, columns // 128, 128)
        x = jnp.swapaxes(x, -3, -2)
        return x.reshape(*lead, rows * (columns // 128), 128)

    def per_device(control, vertical_modes, mode_counts, perturbations, slot_index, blend_weight):
        members, slots, levels = perturbations.shape[:3]
        windows = slot_index.shape[0]
        ctrl = folded(control).reshape(-1, 128)
        pert = folded(perturbations).reshape(members, slots, levels // 2, 16, 128)
        rows = ctrl.shape[0]
        nc = CHUNKS
        lc = levels // n_mem // nc
        f32 = jnp.float32
        slot = (nc, slots, lc, 8, 128)
        one = (nc, lc, 8, 128)
        vmem = pl.BlockSpec(memory_space=pltpu.VMEM)
        hbm = pl.BlockSpec(memory_space=pl.ANY)
        dma = pltpu.SemaphoreType.DMA
        regular = pltpu.SemaphoreType.REGULAR
        gath, scale = pl.pallas_call(
            functools.partial(kernel, n_tm, n_mem, n_tile, members, windows),
            out_shape=(
                pltpu.VMEM((n_mem, nc, 3, lc, 8, 128), f32),
                pltpu.VMEM((windows, 2, 8, 128), f32),
            ),
            in_specs=[hbm] * 6,
            out_specs=(vmem, vmem),
            scratch_shapes=[
                pltpu.VMEM((3, rows, 128), f32),
                pltpu.VMEM(pert.shape, jnp.bfloat16),
                pltpu.VMEM((rows, 128), f32),
                pltpu.VMEM(slot, f32), pltpu.VMEM(slot, f32), pltpu.VMEM(slot, f32),
                pltpu.VMEM(one, f32), pltpu.VMEM(one, f32),
                pltpu.VMEM(slot, f32), pltpu.VMEM(slot, f32),
                pltpu.VMEM(one, f32), pltpu.VMEM(one, f32), pltpu.VMEM(one, f32),
                pltpu.SMEM((2, levels), f32), pltpu.SMEM(mode_counts.shape, jnp.int32),
                pltpu.SMEM((windows,), jnp.int32), pltpu.SMEM((windows,), f32),
                dma((6,)), dma((2,)), dma((2,)), dma((13, nc)), dma((13, nc)), regular, regular,
            ],
            compiler_params=pltpu.CompilerParams(collective_id=0, has_side_effects=True),
        )(ctrl, pert, vertical_modes.T, mode_counts, slot_index, blend_weight)
        out = pl.pallas_call(
            blend_kernel,
            out_shape=jax.ShapeDtypeStruct((windows, levels, 8, 128), f32),
            in_specs=[vmem, vmem],
            out_specs=hbm,
            scratch_shapes=[pltpu.VMEM((windows, levels, 8, 128), f32), dma((windows,))],
        )(*(pltpu.with_memory_space_constraint(x, pltpu.VMEM) for x in (gath, scale)))
        out = out.reshape(windows, levels, 2, 4, 128)
        return jnp.swapaxes(out, -3, -2).reshape(windows, levels, 4, 256)

    return jax.shard_map(
        per_device,
        mesh=mesh,
        in_specs=(
            P("mem", None, "tile", None), P(), P("tile"),
            P("mem", "tm", None, "tile", None), P("tm"), P("tm"),
        ),
        out_specs=P("tm", None, "tile", None),
        check_vma=False,
    )
```

```python
import functools
import math
from contextlib import nullcontext as scope

import jax
import jax.numpy as jnp
from jax import lax
from jax.experimental import pallas as pl
from jax.experimental.pallas import tpu as pltpu
from jax.sharding import PartitionSpec as P

SMOOTH = 4
DIFFUSION = 0.24
CHUNKS = 8
DIRECT = 3
MESH = pl.DeviceIdType.MESH


def smooth_group(halo, f_ref, counts, norm, group, rows):
    lane = lax.broadcasted_iota(jnp.int32, (rows, 128), 1)
    first, last = lane == 0, lane == 127
    base = group * 64

    def load(x, h):
        tile, inner = (x + 4) // 4, x % 4
        return halo[tile, pl.ds(base + h * 4 + inner, rows, 8), :]

    field = {(x, h): load(x, h) for x in range(-4, 8) for h in range(2)}
    for step in range(SMOOTH):
        lo, hi = -3 + step, 7 - step
        new = {}
        for x in range(lo, hi):
            pair = [field[x, 0], field[x, 1]]
            up = [pltpu.roll(v, 1, 1) for v in pair]
            down = [pltpu.roll(v, 127, 1) for v in pair]
            lateral = [
                jnp.where(first, 0.0, up[0]) + jnp.where(last, down[1], down[0]),
                jnp.where(first, up[0], up[1]) + jnp.where(last, 0.0, down[1]),
            ]
            for h in range(2):
                near = field[x - 1, h] + field[x + 1, h]
                new[x, h] = (1.0 - 4.0 * DIFFUSION) * pair[h] + DIFFUSION * (
                    near + lateral[h]
                )
        field = new
    mode = lax.broadcasted_iota(jnp.int32, (rows, 128), 0) % 2
    for x in range(4):
        scales = [jnp.where(m < counts[x], norm, 0.0) for m in range(2)]
        scale = jnp.where(mode == 0, scales[0], scales[1])
        for h in range(2):
            f_ref[pl.ds(base + h * 4 + x, rows, 8), :] = field[x, h] * scale


def kernel(
    n_tm, n_mem, n_tile, members, windows,
    ctrl, pert_hbm, modes_hbm, counts_hbm, index_hbm, weight_hbm,
    gath, scale,
    halo, pert, f_ref, far, near, mail_far, mail,
    za_out, za_in, zb_in, modes, counts, slot_index, weight,
    load_sems, halo_sems, send, recv, recv_all, ready_next, ready_back,
):
    t, m = lax.axis_index("tm"), lax.axis_index("mem")
    tile = lax.axis_index("tile")
    nc = far.shape[0]
    lc = far.shape[2]
    pairs = lc // 2
    quarter_pairs = nc * pairs
    norm = 1.0 / math.sqrt(members * n_mem - 1)

    mem_r, mem_l = lax.rem(m + 1, n_mem), lax.rem(m + n_mem - 1, n_mem)
    mem_f = lax.rem(m + 2, n_mem)
    tm_r, tm_l = lax.rem(t + 1, n_tm), lax.rem(t + n_tm - 1, n_tm)
    right, left, across = {"mem": mem_r}, {"mem": mem_l}, {"mem": mem_f}
    onward, back = {"tm": tm_r}, {"tm": tm_l}
    run = n_tile // 4
    place = lax.rem(tile, run)
    tile_r, tile_l = lax.rem(tile + 1, n_tile), lax.rem(tile + n_tile - 1, n_tile)
    head, tail = place == 0, place == run - 1
    low, high = t == 0, t == n_tm - 1
    step_r = jnp.where(tail & jnp.logical_not(high), tm_r, t)
    step_l = jnp.where(head & jnp.logical_not(low), tm_l, t)
    next_tile = {"tm": step_r, "tile": tile_r}
    last_tile = {"tm": step_l, "tile": tile_l}

    def signal(sem, device):
        pl.semaphore_signal(sem, inc=1, device_id=device, device_id_type=MESH)

    barrier = pltpu.get_barrier_semaphore()
    partners = (next_tile, last_tile, right, left, across)
    for partner in partners:
        signal(barrier, partner)

    @pl.when(t < 2)
    def _():
        signal(barrier, onward)

    @pl.when((t == 0) | (t == 3))
    def _():
        signal(barrier, back)

    loads = [
        pltpu.make_async_copy(src, dst, load_sems.at[k])
        for k, (src, dst) in enumerate((
            (ctrl, halo.at[1]), (counts_hbm, counts), (modes_hbm, modes),
            (index_hbm, slot_index), (weight_hbm, weight), (pert_hbm, pert),
        ))
    ]
    for load in loads:
        load.start()
    with scope("barrier"):
        loads[0].wait()
        extra = jnp.where(t == 0, 0, jnp.where(t == 2, 2, 1))
        extra += jnp.where((low & tail) | (high & head), 1, 0)
        extra -= jnp.where((low & head) | (high & tail), 1, 0)
        pl.semaphore_wait(barrier, len(partners) + extra)

    def remote(src, dst, s, r, device):
        return pltpu.make_async_remote_copy(
            src_ref=src, dst_ref=dst, send_sem=s, recv_sem=r,
            device_id=device, device_id_type=MESH,
        )

    def to_right(device):
        return remote(halo.at[1], halo.at[0], halo_sems.at[0], halo_sems.at[1], device)

    def to_left(device):
        return remote(halo.at[1], halo.at[2], halo_sems.at[2], halo_sems.at[3], device)

    def to_both_tm(copy):
        return remote(halo.at[1], copy[0], halo_sems.at[4], copy[1], copy[2])

    wrap_r = to_both_tm((halo.at[0], halo_sems.at[1], {"tile": tile_r}))
    wrap_l = to_both_tm((halo.at[2], halo_sems.at[3], {"tile": tile_l}))
    sends_r = jnp.logical_not(high & tail)
    sends_l = jnp.logical_not(low & head)

    @pl.when(sends_r)
    def _():
        to_right(next_tile).start()

    @pl.when(sends_l)
    def _():
        to_left(last_tile).start()

    @pl.when(low & tail)
    def _():
        wrap_r.start()

    @pl.when(high & head)
    def _():
        wrap_l.start()

    @pl.when((t == 1) | (t == 2))
    def _():
        signal(ready_next, back)

    @pl.when(t >= 2)
    def _():
        signal(ready_back, onward)

    for load in loads[1:5]:
        load.wait()
    for w in range(windows):
        b = weight[w]
        later = slot_index[w] - 2 * t == 1
        scale[w, 0] = jnp.full((8, 128), jnp.where(later, 1.0, b), jnp.float32)
        scale[w, 1] = jnp.full((8, 128), jnp.where(later, b, 0.0), jnp.float32)

    @pl.when(t == 0)
    def _():
        def clear(i, carry):
            gath[i // nc, lax.rem(i, nc), 2] = jnp.zeros_like(za_out[0])
            return carry

        lax.fori_loop(0, n_mem * nc, clear, 0)

    with scope("halo"):
        to_right(next_tile).wait_recv()
        to_left(last_tile).wait_recv()

    with scope("smooth"):
        fields = 2 * members
        for group in range(0, fields, 8):
            smooth_group(halo, f_ref, counts, norm, group // 8, min(8, fields - group))
        loads[5].wait()

    def part(quarter, chunk, dst):
        def body(p, carry):
            lp = quarter * quarter_pairs + chunk * pairs + p
            v = [[modes[mode, 2 * lp + j] for mode in range(2)] for j in range(2)]
            acc = [[None, None], [None, None]]
            for k in range(members):
                f0 = f_ref[pl.ds(16 * k, 8), :]
                f1 = f_ref[pl.ds(16 * k + 8, 8), :]
                loc = [v[j][0] * f0 + v[j][1] * f1 for j in range(2)]
                for s in range(2):
                    x = pert[k, s, lp].astype(jnp.float32)
                    for j in range(2):
                        term = loc[j] * x[8 * j : 8 * j + 8]
                        acc[s][j] = term if k == 0 else acc[s][j] + term
            for s in range(2):
                for j in range(2):
                    dst[s, 2 * p + j] = acc[s][j]
            return carry

        if pairs == 1:
            body(0, 0)
        else:
            lax.fori_loop(0, pairs, body, 0)

    def channel(k, c, src, dst, device):
        arrived = recv_all.at[k - 5] if k >= 5 else recv.at[k, c]
        return remote(src, dst, send.at[k], arrived, device)

    def arrive(k, c, size):
        channel(k, c, size, size, right).wait_recv()

    def sent(k, size):
        channel(k, 0, size, size, right).wait_send()

    def both(ref):
        return ref.at[pl.ds(0, 2)]

    def chain(c):
        return channel(2, c, za_out.at[c], za_in.at[c], onward)

    def around(c):
        return channel(3, c, za_out.at[c], zb_in.at[c], back)

    def relay(c):
        return channel(3, c, zb_in.at[c], zb_in.at[c], back)

    direct = range(DIRECT)
    ringed = range(DIRECT, nc)

    def send_near(c, side):
        channel(1, c, near.at[c, side], mail.at[c, side], (right, left)[side]).start()

    with scope("far"):
        for c in direct:
            part(mem_f, c, far.at[c])
            remote(far.at[c], mail.at[c, 2], send.at[0], recv.at[1, c], across).start()
            part(mem_r, c, near.at[c, 0])
            send_near(c, 0)
            part(mem_l, c, near.at[c, 1])
            send_near(c, 1)
        for c in ringed:
            part(mem_f, c, far.at[c])
            channel(0, c, far.at[c, 0], mail_far.at[c, 0], right).start()
            channel(0, c, far.at[c, 1], mail_far.at[c, 1], left).start()
    with scope("near"):
        for c in ringed:
            part(mem_r, c, near.at[c, 0])
            part(mem_l, c, near.at[c, 1])
        for c in range(nc):
            part(m, c, gath.at[m, c])

    def step_a(c):
        arrive(0, c, mail_far.at[c])
        near[c, 0, 0] += mail_far[c, 0]
        send_near(c, 0)
        near[c, 1, 1] += mail_far[c, 1]
        send_near(c, 1)

    def step_b(c):
        sources = 3 if c < DIRECT else 2
        arrive(1, c, mail.at[c, pl.ds(0, sources)])
        for level in range(lc):
            total = None
            for s in range(2):
                value = mail[c, 0, s, level] + mail[c, 1, s, level]
                if sources == 3:
                    value = value + mail[c, 2, s, level]
                value = gath[m, c, s, level] + value
                gath[m, c, s, level] = value
                total = value if s == 0 else total + value
            za_out[c, level] = total

        if c == 0:
            @pl.when(t < 2)
            def _():
                pl.semaphore_wait(ready_next, 1)

            @pl.when((t == 0) | (t == 3))
            def _():
                pl.semaphore_wait(ready_back, 1)

        @pl.when(t < 2)
        def _():
            chain(c).start()

        @pl.when(t == 0)
        def _():
            around(c).start()

    def step_g(c):
        for device in (right, left):
            channel(4, c, both(gath.at[m, c]), both(gath.at[m, c]), device).start()

    def step_z2(c):
        chain(c).wait_recv()
        za_out[c] += za_in[c]
        chain(c).start()

    def step_z3(c):
        around(c).wait_recv()
        relay(c).start()

    def step_d(c):
        arrive(4, c, near.at[c])
        channel(5, c, gath.at[mem_l, c, 0], gath.at[mem_l, c, 0], right).start()
        channel(5, c, gath.at[mem_r, c, 1], gath.at[mem_r, c, 1], left).start()

    def early_1(c):
        chain(c).wait_recv()
        gath[m, c, 2] = za_in[c]

    def early_2(c):
        relay(c).wait_recv()
        gath[m, c, 2] = za_in[c] + zb_in[c]

    def early_3(c):
        chain(c).wait_recv()
        gath[m, c, 2] = za_in[c] + zb_in[c]

    def step_e(c, early):
        early(c)
        for device in (across, right, left):
            channel(6, c, gath.at[m, c, 2], gath.at[m, c, 2], device).start()

    def run(steps):
        for step, *args in steps:
            with scope(f"{step.__name__.replace("step_","").upper()[0]}{args[0]}"):
                step(*args)

    every = range(nc)
    first = [(step_a, c) for c in ringed[:1]]
    for k in range(max(DIRECT, nc - DIRECT - 1)):
        if DIRECT + 1 + k < nc:
            first.append((step_a, DIRECT + 1 + k))
        if k < DIRECT:
            first.append((step_b, k))
    run(first)

    @pl.when(t < 2)
    def _():
        run([(step_b, c) for c in ringed] + [(step_g, c) for c in every] + [(step_d, c) for c in every])

    @pl.when(t == 1)
    def _():
        run([(step_e, c, early_1) for c in every])

    @pl.when(t == 2)
    def _():
        run([(step_z2, c) for c in direct] + [(step_b, c) for c in ringed])
        run([(step_g, c) for c in every] + [(step_z2, c) for c in ringed])
        for c in every:
            run([(step_e, c, early_2), (step_d, c)])

    @pl.when(t == 3)
    def _():
        run([(step_z3, c) for c in direct])
        for c in ringed:
            run([(step_b, c), (step_z3, c)])
        run([(step_g, c) for c in every] + [(step_d, c) for c in every])
        run([(step_e, c, early_3) for c in every])

    with scope("P"):
        arrive(5, 0, far)
    with scope("H"):
        @pl.when(t > 0)
        def _():
            arrive(6, 0, gath.at[0])

    with scope("W"):
        @pl.when(sends_r)
        def _():
            to_right(next_tile).wait_send()

        @pl.when(sends_l)
        def _():
            to_left(last_tile).wait_send()

        @pl.when((low & tail) | (high & head))
        def _():
            wrap_r.wait_send()

        sent(0, far)
        sent(1, near)
        sent(4, near)
        sent(5, far)

        @pl.when(t < 3)
        def _():
            sent(2, za_out)

        @pl.when((t == 0) | (t == 3))
        def _():
            sent(3, za_out)

        @pl.when(t > 0)
        def _():
            sent(6, gath.at[0])


def blend_kernel(gath, scale, out, block, sems):
    n_mem, nc, _, lc = gath.shape[:4]
    windows = block.shape[0]
    copies = []
    for w in range(windows):
        a, b = scale[w, 0], scale[w, 1]
        for q in range(n_mem):
            for c in range(nc):
                for level in range(lc):
                    r0, r1, e = (gath[q, c, i, level] for i in range(3))
                    block[w, (q * nc + c) * lc + level] = e + (a * r0 + b * r1)
        copies.append(pltpu.make_async_copy(block.at[w], out.at[w], sems.at[w]))
        copies[-1].start()
    for copy in copies:
        copy.wait()


def solution(mesh):
    n_tm, n_mem, n_tile = (mesh.shape[a] for a in ("tm", "mem", "tile"))

    def folded(x):
        *lead, rows, columns = x.shape
        x = x.reshape(*lead, rows, columns // 128, 128)
        x = jnp.swapaxes(x, -3, -2)
        return x.reshape(*lead, rows * (columns // 128), 128)

    def per_device(control, vertical_modes, mode_counts, perturbations, slot_index, blend_weight):
        members, slots, levels = perturbations.shape[:3]
        windows = slot_index.shape[0]
        ctrl = folded(control).reshape(-1, 128)
        pert = folded(perturbations).reshape(members, slots, levels // 2, 16, 128)
        rows = ctrl.shape[0]
        nc = CHUNKS
        lc = levels // n_mem // nc
        f32 = jnp.float32
        slot = (nc, slots, lc, 8, 128)
        one = (nc, lc, 8, 128)
        vmem = pl.BlockSpec(memory_space=pltpu.VMEM)
        hbm = pl.BlockSpec(memory_space=pl.ANY)
        dma = pltpu.SemaphoreType.DMA
        regular = pltpu.SemaphoreType.REGULAR
        gath, scale = pl.pallas_call(
            functools.partial(kernel, n_tm, n_mem, n_tile, members, windows),
            out_shape=(
                pltpu.VMEM((n_mem, nc, 3, lc, 8, 128), f32),
                pltpu.VMEM((windows, 2, 8, 128), f32),
            ),
            in_specs=[hbm] * 6,
            out_specs=(vmem, vmem),
            scratch_shapes=[
                pltpu.VMEM((3, rows, 128), f32),
                pltpu.VMEM(pert.shape, jnp.bfloat16),
                pltpu.VMEM((rows, 128), f32),
                pltpu.VMEM(slot, f32), pltpu.VMEM((nc, 2, *slot[1:]), f32),
                pltpu.VMEM(slot, f32), pltpu.VMEM((nc, 3, *slot[1:]), f32),
                pltpu.VMEM(one, f32), pltpu.VMEM(one, f32), pltpu.VMEM(one, f32),
                pltpu.SMEM((2, levels), f32), pltpu.SMEM(mode_counts.shape, jnp.int32),
                pltpu.SMEM((windows,), jnp.int32), pltpu.SMEM((windows,), f32),
                dma((6,)), dma((5,)), dma((7,)), dma((5, nc)), dma((2,)), regular, regular,
            ],
            compiler_params=pltpu.CompilerParams(collective_id=0, has_side_effects=True),
        )(ctrl, pert, vertical_modes.T, mode_counts, slot_index, blend_weight)
        out = pl.pallas_call(
            blend_kernel,
            out_shape=jax.ShapeDtypeStruct((windows, levels, 8, 128), f32),
            in_specs=[vmem, vmem],
            out_specs=hbm,
            scratch_shapes=[pltpu.VMEM((windows, levels, 8, 128), f32), dma((windows,))],
        )(*(pltpu.with_memory_space_constraint(x, pltpu.VMEM) for x in (gath, scale)))
        out = out.reshape(windows, levels, 2, 4, 128)
        return jnp.swapaxes(out, -3, -2).reshape(windows, levels, 4, 256)

    return jax.shard_map(
        per_device,
        mesh=mesh,
        in_specs=(
            P("mem", None, "tile", None), P(), P("tile"),
            P("mem", "tm", None, "tile", None), P("tm"), P("tm"),
        ),
        out_specs=P("tm", None, "tile", None),
        check_vma=False,
    )
```

```python
import functools
import math
from contextlib import nullcontext as scope

import jax
import jax.numpy as jnp
from jax import lax
from jax.experimental import pallas as pl
from jax.experimental.pallas import tpu as pltpu
from jax.sharding import PartitionSpec as P

SMOOTH = 4
DIFFUSION = 0.24
CHUNKS = 8
HOP = 1
DIRECT = 3
MESH = pl.DeviceIdType.MESH


def smooth_group(halo, f_ref, counts, norm, group, rows):
    lane = lax.broadcasted_iota(jnp.int32, (rows, 128), 1)
    first, last = lane == 0, lane == 127
    base = group * 64

    def load(x, h):
        tile, inner = (x + 4) // 4, x % 4
        return halo[tile, pl.ds(base + h * 4 + inner, rows, 8), :]

    field = {(x, h): load(x, h) for x in range(-4, 8) for h in range(2)}
    for step in range(SMOOTH):
        lo, hi = -3 + step, 7 - step
        new = {}
        for x in range(lo, hi):
            pair = [field[x, 0], field[x, 1]]
            up = [pltpu.roll(v, 1, 1) for v in pair]
            down = [pltpu.roll(v, 127, 1) for v in pair]
            lateral = [
                jnp.where(first, 0.0, up[0]) + jnp.where(last, down[1], down[0]),
                jnp.where(first, up[0], up[1]) + jnp.where(last, 0.0, down[1]),
            ]
            for h in range(2):
                near = field[x - 1, h] + field[x + 1, h]
                new[x, h] = (1.0 - 4.0 * DIFFUSION) * pair[h] + DIFFUSION * (
                    near + lateral[h]
                )
        field = new
    mode = lax.broadcasted_iota(jnp.int32, (rows, 128), 0) % 2
    for x in range(4):
        scales = [jnp.where(m < counts[x], norm, 0.0) for m in range(2)]
        scale = jnp.where(mode == 0, scales[0], scales[1])
        for h in range(2):
            f_ref[pl.ds(base + h * 4 + x, rows, 8), :] = field[x, h] * scale


def kernel(
    n_tm, n_mem, n_tile, members, windows,
    ctrl, pert_hbm, modes_hbm, counts_hbm, index_hbm, weight_hbm,
    gath, scale,
    halo, pert, f_ref, far, near, mail_far, mail,
    za_out, za_in, zb_in, zc_in, modes, counts, slot_index, weight,
    load_sems, halo_sems, send, recv, ready_next, ready_back,
):
    t, m = lax.axis_index("tm"), lax.axis_index("mem")
    tile = lax.axis_index("tile")
    nc = far.shape[0]
    lc = far.shape[2]
    pairs = lc // 2
    quarter_pairs = nc * pairs
    norm = 1.0 / math.sqrt(members * n_mem - 1)

    mem_r, mem_l = lax.rem(m + 1, n_mem), lax.rem(m + n_mem - 1, n_mem)
    mem_f = lax.rem(m + 2, n_mem)
    tm_r, tm_l = lax.rem(t + 1, n_tm), lax.rem(t + n_tm - 1, n_tm)
    right, left, across = {"mem": mem_r}, {"mem": mem_l}, {"mem": mem_f}
    onward, back = {"tm": tm_r}, {"tm": tm_l}
    run = n_tile // 4
    place = lax.rem(tile, run)
    tile_r, tile_l = lax.rem(tile + 1, n_tile), lax.rem(tile + n_tile - 1, n_tile)
    head, tail = place == 0, place == run - 1
    low, high, odd = t == 0, t == n_tm - 1, lax.rem(t, 2) == 1
    step_r = jnp.where(tail & jnp.logical_not(odd), tm_r, t)
    step_l = jnp.where(head & jnp.logical_not(low), tm_l, t)
    next_tile = {"tm": step_r, "tile": tile_r}
    last_tile = {"tm": step_l, "tile": tile_l}

    def signal(sem, device):
        pl.semaphore_signal(sem, inc=1, device_id=device, device_id_type=MESH)

    barrier = pltpu.get_barrier_semaphore()
    partners = (next_tile, last_tile, right, left, across)
    for partner in partners:
        signal(barrier, partner)

    @pl.when(t < 2)
    def _():
        signal(barrier, onward)

    @pl.when((t == 0) | (t == 3))
    def _():
        signal(barrier, back)

    loads = [
        pltpu.make_async_copy(src, dst, load_sems.at[k])
        for k, (src, dst) in enumerate((
            (ctrl, halo.at[1]), (counts_hbm, counts), (modes_hbm, modes),
            (index_hbm, slot_index), (weight_hbm, weight), (pert_hbm, pert),
        ))
    ]
    for load in loads:
        load.start()
    with scope("barrier"):
        loads[0].wait()
        extra = jnp.where(t == 0, 0, jnp.where(t == 2, 2, 1))
        extra += jnp.where((low & tail) | (odd & head), 1, 0)
        extra -= jnp.where((jnp.logical_not(odd) & head) | (high & tail), 1, 0)
        pl.semaphore_wait(barrier, len(partners) + extra)

    def remote(src, dst, s, r, device):
        return pltpu.make_async_remote_copy(
            src_ref=src, dst_ref=dst, send_sem=s, recv_sem=r,
            device_id=device, device_id_type=MESH,
        )

    def to_right(device):
        return remote(halo.at[1], halo.at[0], halo_sems.at[0], halo_sems.at[1], device)

    def to_left(device):
        return remote(halo.at[1], halo.at[2], halo_sems.at[2], halo_sems.at[3], device)

    def to_both_tm(copy):
        return remote(halo.at[1], copy[0], halo_sems.at[4], copy[1], copy[2])

    wrap_r = to_both_tm((halo.at[0], halo_sems.at[1], {"tile": tile_r}))
    wrap_l = to_both_tm((halo.at[2], halo_sems.at[3], {"tile": tile_l}))
    sends_r = jnp.logical_not(high & tail)
    sends_l = jnp.logical_not(head & jnp.logical_not(odd))
    right_tile = {"tm": jnp.where(tail, tm_r, t), "tile": tile_r}

    @pl.when(sends_r)
    def _():
        to_right(right_tile).start()

    @pl.when(sends_l)
    def _():
        to_left(last_tile).start()

    @pl.when(low & tail)
    def _():
        wrap_r.start()

    @pl.when(odd & head)
    def _():
        wrap_l.start()

    @pl.when((t == 1) | (t == 2))
    def _():
        signal(ready_next, back)

    @pl.when(t >= 2)
    def _():
        signal(ready_back, onward)

    for load in loads[1:5]:
        load.wait()
    for w in range(windows):
        b = weight[w]
        later = slot_index[w] - 2 * t == 1
        scale[w, 0] = jnp.full((8, 128), jnp.where(later, 1.0, b), jnp.float32)
        scale[w, 1] = jnp.full((8, 128), jnp.where(later, b, 0.0), jnp.float32)

    @pl.when(t == 0)
    def _():
        def clear(i, carry):
            gath[i // nc, lax.rem(i, nc), 2] = jnp.zeros((lc, 8, 128), jnp.float32)
            return carry

        lax.fori_loop(0, n_mem * nc, clear, 0)

    with scope("halo"):
        to_right(next_tile).wait_recv()
        to_left(last_tile).wait_recv()

    with scope("smooth"):
        fields = 2 * members
        for group in range(0, fields, 8):
            smooth_group(halo, f_ref, counts, norm, group // 8, min(8, fields - group))
        loads[5].wait()

    def part(quarter, chunk, dst):
        def body(p, carry):
            lp = quarter * quarter_pairs + chunk * pairs + p
            v = [[modes[mode, 2 * lp + j] for mode in range(2)] for j in range(2)]
            acc = [[None, None], [None, None]]
            for k in range(members):
                f0 = f_ref[pl.ds(16 * k, 8), :]
                f1 = f_ref[pl.ds(16 * k + 8, 8), :]
                loc = [v[j][0] * f0 + v[j][1] * f1 for j in range(2)]
                for s in range(2):
                    x = pert[k, s, lp].astype(jnp.float32)
                    for j in range(2):
                        term = loc[j] * x[8 * j : 8 * j + 8]
                        acc[s][j] = term if k == 0 else acc[s][j] + term
            for s in range(2):
                for j in range(2):
                    dst[s, 2 * p + j] = acc[s][j]
            return carry

        if pairs == 1:
            body(0, 0)
        else:
            lax.fori_loop(0, pairs, body, 0)

    late = place >= run - 2

    half = nc // 2
    hops = nc * lc // HOP
    bases = (-DIRECT, nc - DIRECT, 2 * nc - DIRECT, 2 * nc - DIRECT + hops)
    bases += (bases[3] + half, bases[3] + half + 2, bases[3] + half + 3)
    bases += (bases[6] + 1,)
    shares = (1, 1, 1, 2, half, nc, nc, 2)

    def channel(k, c, src, dst, device):
        return remote(src, dst, send.at[k], recv.at[bases[k] + c // shares[k]], device)

    def arrive(k, c, size):
        channel(k, c, size, size, right).wait_recv()

    def sent(k, size):
        remote(size, size, send.at[k], recv.at[0], right).wait_send()

    def both(ref):
        return ref.at[pl.ds(0, 2)]

    def units(c):
        return [u for u in range(nc * lc // HOP) if c * lc < (u + 1) * HOP <= (c + 1) * lc]

    def chain(u):
        own = pl.ds(u * HOP, HOP)
        return channel(2, u, za_out.at[own], za_in.at[own], onward)

    def around(c):
        two = pl.ds((c - 1) * lc, 2 * lc)
        return channel(3, c, za_out.at[two], zb_in.at[two], back)

    def relay(c):
        two = pl.ds((c - 1) * lc, 2 * lc)
        return channel(3, c, zb_in.at[two], zb_in.at[two], back)

    def bypass(c):
        two = pl.ds((c - 1) * lc, 2 * lc)
        return channel(7, c, zb_in.at[two], zc_in.at[two], back)

    direct = range(DIRECT)
    ringed = range(DIRECT, nc)

    def send_near(c, side):
        channel(1, c, near.at[c, side], mail.at[c, side], (right, left)[side]).start()

    with scope("far"):
        for c in ringed:
            part(mem_f, c, far.at[c])
            channel(0, c, far.at[c, 0], mail_far.at[c, 0], right).start()
            channel(0, c, far.at[c, 1], mail_far.at[c, 1], left).start()
        for c in direct:
            part(mem_f, c, far.at[c])
            remote(far.at[c], mail.at[c, 2], send.at[0], recv.at[bases[1] + c], across).start()
            part(mem_r, c, near.at[c, 0])
            send_near(c, 0)
            part(mem_l, c, near.at[c, 1])
            send_near(c, 1)
    with scope("near"):
        for c in ringed:
            part(mem_r, c, near.at[c, 0])
            part(mem_l, c, near.at[c, 1])
        for c in range(nc):
            part(m, c, gath.at[m, c])

    def step_a(c):
        arrive(0, c, mail_far.at[c])
        near[c, 0, 0] += mail_far[c, 0]
        send_near(c, 0)
        near[c, 1, 1] += mail_far[c, 1]
        send_near(c, 1)

    def step_b(c):
        sources = 3 if c < DIRECT else 2
        arrive(1, c, mail.at[c, pl.ds(0, sources)])
        for level in range(lc):
            total = None
            for s in range(2):
                value = mail[c, 0, s, level] + mail[c, 1, s, level]
                if sources == 3:
                    value = value + mail[c, 2, s, level]
                value = gath[m, c, s, level] + value
                gath[m, c, s, level] = value
                total = value if s == 0 else total + value
            za_out[c * lc + level] = total

        if c == 0:
            @pl.when(t < 2)
            def _():
                pl.semaphore_wait(ready_next, 1)

            @pl.when((t == 0) | (t == 3))
            def _():
                pl.semaphore_wait(ready_back, 1)

        @pl.when((t < 2) | (late & (t == 2)))
        def _():
            for u in units(c):
                chain(u).start()

        if c % 2 == 1:
            @pl.when((t == 0) | (late & (t == 1)))
            def _():
                around(c).start()

    def step_g(c):
        own = both(gath.at[m, c])
        for device in (right, left):
            channel(4, c, own, own, device).start()
        if c >= half:
            remote(own, own, send.at[5], recv.at[bases[4] + 1], across).start()

    def step_z2(c):
        for u in units(c):
            chain(u).wait_recv()
            for level in range(u * HOP, (u + 1) * HOP):
                za_out[level] += za_in[level]
            chain(u).start()

    def step_z3(c):
        if c % 2 == 1:
            around(c).wait_recv()
            relay(c).start()

    def step_d():
        arrive(4, 0, near.at[pl.ds(0, half)])
        for c in range(half):
            channel(5, 0, gath.at[mem_l, c, 0], gath.at[mem_l, c, 0], right).start()
            channel(5, 0, gath.at[mem_r, c, 1], gath.at[mem_r, c, 1], left).start()

    def early_1(level):
        return za_in[level]

    def early_23(level):
        return za_in[level] + zb_in[level]

    def step_e(c, early):
        def come():
            for u in units(c):
                chain(u).wait_recv()

        if early is early_23 and c % 2 == 0:
            @pl.when(t == 2)
            def _():
                relay(c + 1).wait_recv()

            @pl.when(late & (t == 3))
            def _():
                bypass(c + 1).wait_recv()

        pl.when((t != 2) | late)(come)
        for level in range(lc):
            gath[m, c, 2, level] = early(c * lc + level)
        if early is early_23:
            @pl.when(late & (t == 3))
            def _():
                for level in range(lc):
                    gath[m, c, 2, level] += zc_in[c * lc + level]

        for device in (across, right, left):
            channel(6, c, gath.at[m, c, 2], gath.at[m, c, 2], device).start()

    def play(steps):
        for step, *args in steps:
            with scope(f"{step.__name__.replace("step_","").upper()[0]}{args[0]}"):
                step(*args)

    every = range(nc)
    first = [(step_a, c) for c in ringed[:1]]
    for k in range(max(DIRECT, nc - DIRECT - 1)):
        if DIRECT + 1 + k < nc:
            first.append((step_a, DIRECT + 1 + k))
        if k < DIRECT:
            first.append((step_b, k))
    play(first)

    def rest(also=None):
        for c in ringed:
            play([(step_b, c)])
            if also is not None:
                play([(also, c)])
            play([(step_g, k) for k in (range(DIRECT + 1) if c == DIRECT else (c,))])

    @pl.when(t == 0)
    def _():
        rest()
        step_d()

        @pl.when(late)
        def _():
            for c in range(1, nc, 2):
                around(c).wait_recv()
                bypass(c).start()

    @pl.when(t == 1)
    def _():
        play([(step_b, c) for c in ringed] + [(step_g, c) for c in every])
        step_d()
        play([(step_e, c, early_1) for c in every])

    @pl.when((t == 2) & jnp.logical_not(late))
    def _():
        play([(step_z2, c) for c in direct])
        rest(step_z2)

    @pl.when((t == 2) & late)
    def _():
        rest()

    @pl.when(t == 2)
    def _():
        play([(step_e, c, early_23) for c in range(half)])
        step_d()
        play([(step_e, c, early_23) for c in range(half, nc)])

    @pl.when(t == 3)
    def _():
        play([(step_z3, c) for c in direct])
        rest(step_z3)
        step_d()
        play([(step_e, c, early_23) for c in every])

    with scope("P"):
        arrive(4, half, mail.at[pl.ds(0, half)])
        arrive(5, 0, far.at[pl.ds(0, half)])
    with scope("H"):
        @pl.when(t > 0)
        def _():
            arrive(6, 0, gath.at[0])

    with scope("W"):
        @pl.when(sends_r)
        def _():
            to_right(right_tile).wait_send()

        @pl.when(sends_l)
        def _():
            to_left(last_tile).wait_send()

        @pl.when((low & tail) | (odd & head))
        def _():
            wrap_r.wait_send()

        sent(0, far)
        sent(1, near)
        sent(4, near)
        sent(5, far)

        @pl.when(t < 3)
        def _():
            sent(2, za_out)

        @pl.when((t == 0) | (t == 3))
        def _():
            sent(3, za_out)

        @pl.when(late & (t == 1))
        def _():
            sent(3, za_out)

        @pl.when(late & (t == 0))
        def _():
            sent(7, za_out)

        @pl.when(t > 0)
        def _():
            sent(6, gath.at[0])


def blend_kernel(gath, scale, out, block, sems):
    n_mem, nc, _, lc = gath.shape[:4]
    windows = block.shape[0]
    copies = []
    for w in range(windows):
        a, b = scale[w, 0], scale[w, 1]
        for q in range(n_mem):
            for c in range(nc):
                for level in range(lc):
                    r0, r1, e = (gath[q, c, i, level] for i in range(3))
                    block[w, (q * nc + c) * lc + level] = e + (a * r0 + b * r1)
        copies.append(pltpu.make_async_copy(block.at[w], out.at[w], sems.at[w]))
        copies[-1].start()
    for copy in copies:
        copy.wait()


def solution(mesh):
    n_tm, n_mem, n_tile = (mesh.shape[a] for a in ("tm", "mem", "tile"))

    def folded(x):
        *lead, rows, columns = x.shape
        x = x.reshape(*lead, rows, columns // 128, 128)
        x = jnp.swapaxes(x, -3, -2)
        return x.reshape(*lead, rows * (columns // 128), 128)

    def per_device(control, vertical_modes, mode_counts, perturbations, slot_index, blend_weight):
        members, slots, levels = perturbations.shape[:3]
        windows = slot_index.shape[0]
        ctrl = folded(control).reshape(-1, 128)
        pert = folded(perturbations).reshape(members, slots, levels // 2, 16, 128)
        rows = ctrl.shape[0]
        nc = CHUNKS
        lc = levels // n_mem // nc
        f32 = jnp.float32
        slot = (nc, slots, lc, 8, 128)
        one = (nc * lc, 8, 128)
        vmem = pl.BlockSpec(memory_space=pltpu.VMEM)
        hbm = pl.BlockSpec(memory_space=pl.ANY)
        dma = pltpu.SemaphoreType.DMA
        regular = pltpu.SemaphoreType.REGULAR
        gath, scale = pl.pallas_call(
            functools.partial(kernel, n_tm, n_mem, n_tile, members, windows),
            out_shape=(
                pltpu.VMEM((n_mem, nc, 3, lc, 8, 128), f32),
                pltpu.VMEM((windows, 2, 8, 128), f32),
            ),
            in_specs=[hbm] * 6,
            out_specs=(vmem, vmem),
            scratch_shapes=[
                pltpu.VMEM((3, rows, 128), f32),
                pltpu.VMEM(pert.shape, jnp.bfloat16),
                pltpu.VMEM((rows, 128), f32),
                pltpu.VMEM(slot, f32), pltpu.VMEM((nc, 2, *slot[1:]), f32),
                pltpu.VMEM(slot, f32), pltpu.VMEM((nc, 3, *slot[1:]), f32),
                pltpu.VMEM(one, f32), pltpu.VMEM(one, f32), pltpu.VMEM(one, f32), pltpu.VMEM(one, f32),
                pltpu.SMEM((2, levels), f32), pltpu.SMEM(mode_counts.shape, jnp.int32),
                pltpu.SMEM((windows,), jnp.int32), pltpu.SMEM((windows,), f32),
                dma((6,)), dma((5,)), dma((8,)), dma((2 * nc - DIRECT + nc * lc // HOP + nc + 4,)), regular, regular,
            ],
            compiler_params=pltpu.CompilerParams(collective_id=0, has_side_effects=True),
        )(ctrl, pert, vertical_modes.T, mode_counts, slot_index, blend_weight)
        out = pl.pallas_call(
            blend_kernel,
            out_shape=jax.ShapeDtypeStruct((windows, levels, 8, 128), f32),
            in_specs=[vmem, vmem],
            out_specs=hbm,
            scratch_shapes=[pltpu.VMEM((windows, levels, 8, 128), f32), dma((windows,))],
        )(*(pltpu.with_memory_space_constraint(x, pltpu.VMEM) for x in (gath, scale)))
        out = out.reshape(windows, levels, 2, 4, 128)
        return jnp.swapaxes(out, -3, -2).reshape(windows, levels, 4, 256)

    return jax.shard_map(
        per_device,
        mesh=mesh,
        in_specs=(
            P("mem", None, "tile", None), P(), P("tile"),
            P("mem", "tm", None, "tile", None), P("tm"), P("tm"),
        ),
        out_specs=P("tm", None, "tile", None),
        check_vma=False,
    )
```

```python
import functools
import math
from contextlib import nullcontext as scope

import jax
import jax.numpy as jnp
from jax import lax
from jax.experimental import pallas as pl
from jax.experimental.pallas import tpu as pltpu
from jax.sharding import PartitionSpec as P

SMOOTH = 4
DIFFUSION = 0.24
CHUNKS = 8
HOP = 1
DIRECT = 3
MESH = pl.DeviceIdType.MESH


def spread():
    a, b = 1.0 - 4.0 * DIFFUSION, DIFFUSION
    weights = [[0.0] * (SMOOTH - d + 1) for d in range(SMOOTH + 1)]
    for k in range(SMOOTH + 1):
        for d in range(k % 2, k + 1, 2):
            outer = math.comb(SMOOTH, k) * b**k * math.comb(k, (k - d) // 2)
            for j in range(SMOOTH - k + 1):
                weights[d][j] += outer * math.comb(SMOOTH - k, j) * a ** (SMOOTH - k - j) * b**j
    return weights


def add_rows(halo, total, group, rows, longitudes):
    weights = spread()
    lane = lax.broadcasted_iota(jnp.int32, (rows, 128), 1)
    first, last = lane == 0, lane == 127
    for x in longitudes:
        tile, inner = (x + 4) // 4, x % 4
        reach = [(r, abs(r - x)) for r in range(4) if abs(r - x) <= SMOOTH]
        pair = [halo[tile, pl.ds(group * 64 + h * 4 + inner, rows, 8), :] for h in range(2)]
        for j in range(SMOOTH - min(d for _, d in reach) + 1):
            if j:
                up = [pltpu.roll(v, 1, 1) for v in pair]
                down = [pltpu.roll(v, 127, 1) for v in pair]
                pair = [
                    jnp.where(first, 0.0, up[0]) + jnp.where(last, down[1], down[0]),
                    jnp.where(first, up[0], up[1]) + jnp.where(last, 0.0, down[1]),
                ]
            for r, d in reach:
                if j <= SMOOTH - d:
                    for h in range(2):
                        term = weights[d][j] * pair[h]
                        total[r, h] = total[r, h] + term if (r, h) in total else term


def smooth_own(halo, own, group, rows):
    total = {}
    add_rows(halo, total, group, rows, range(4))
    for (x, h), value in total.items():
        own[group * 8 + h * 4 + x, pl.ds(0, rows)] = value


def smooth_rest(halo, own, f_ref, counts, norm, group, rows):
    total = {
        (x, h): own[group * 8 + h * 4 + x, pl.ds(0, rows)] for x in range(4) for h in range(2)
    }
    add_rows(halo, total, group, rows, (-4, -3, -2, -1, 4, 5, 6, 7))
    mode = lax.broadcasted_iota(jnp.int32, (rows, 128), 0) % 2
    for x in range(4):
        scales = [jnp.where(m < counts[x], norm, 0.0) for m in range(2)]
        scale = jnp.where(mode == 0, scales[0], scales[1])
        for h in range(2):
            f_ref[pl.ds(group * 64 + h * 4 + x, rows, 8), :] = total[x, h] * scale


def kernel(
    n_tm, n_mem, n_tile, members, windows,
    ctrl, pert_hbm, modes_hbm, counts_hbm, index_hbm, weight_hbm,
    gath, scale,
    halo, own, pert, f_ref, far, near, mail_far, mail,
    za_out, za_in, zb_in, zc_in, modes, counts, slot_index, weight,
    halo_sems, send, recv, ready_next, ready_back,
):
    t, m = lax.axis_index("tm"), lax.axis_index("mem")
    tile = lax.axis_index("tile")
    nc = far.shape[0]
    lc = far.shape[2]
    pairs = lc // 2
    quarter_pairs = nc * pairs
    norm = 1.0 / math.sqrt(members * n_mem - 1)

    mem_r, mem_l = lax.rem(m + 1, n_mem), lax.rem(m + n_mem - 1, n_mem)
    mem_f = lax.rem(m + 2, n_mem)
    tm_r, tm_l = lax.rem(t + 1, n_tm), lax.rem(t + n_tm - 1, n_tm)
    right, left, across = {"mem": mem_r}, {"mem": mem_l}, {"mem": mem_f}
    onward, back = {"tm": tm_r}, {"tm": tm_l}
    run = n_tile // 4
    place = lax.rem(tile, run)
    tile_r, tile_l = lax.rem(tile + 1, n_tile), lax.rem(tile + n_tile - 1, n_tile)
    head, tail = place == 0, place == run - 1
    low, high, odd = t == 0, t == n_tm - 1, lax.rem(t, 2) == 1
    step_r = jnp.where(tail & jnp.logical_not(odd), tm_r, t)
    step_l = jnp.where(head & jnp.logical_not(low), tm_l, t)
    next_tile = {"tm": step_r, "tile": tile_r}
    last_tile = {"tm": step_l, "tile": tile_l}

    def signal(sem, device):
        pl.semaphore_signal(sem, inc=1, device_id=device, device_id_type=MESH)

    barrier = pltpu.get_barrier_semaphore()
    partners = (next_tile, last_tile, right, left, across)
    for partner in partners:
        signal(barrier, partner)

    @pl.when(t < 2)
    def _():
        signal(barrier, onward)

    @pl.when((t == 0) | (t == 3))
    def _():
        signal(barrier, back)

    loads = [
        pltpu.make_async_copy(src, dst, send.at[k])
        for k, (src, dst) in enumerate((
            (ctrl, halo.at[1]), (counts_hbm, counts), (modes_hbm, modes),
            (index_hbm, slot_index), (weight_hbm, weight), (pert_hbm, pert),
        ))
    ]
    for load in loads:
        load.start()
    with scope("barrier"):
        loads[0].wait()
        extra = jnp.where(t == 0, 0, jnp.where(t == 2, 2, 1))
        extra += jnp.where((low & tail) | (odd & head), 1, 0)
        extra -= jnp.where((jnp.logical_not(odd) & head) | (high & tail), 1, 0)
        pl.semaphore_wait(barrier, len(partners) + extra)

    def remote(src, dst, s, r, device):
        return pltpu.make_async_remote_copy(
            src_ref=src, dst_ref=dst, send_sem=s, recv_sem=r,
            device_id=device, device_id_type=MESH,
        )

    def to_right(device):
        return remote(halo.at[1], halo.at[0], halo_sems.at[0], halo_sems.at[1], device)

    def to_left(device):
        return remote(halo.at[1], halo.at[2], halo_sems.at[2], halo_sems.at[3], device)

    def to_both_tm(copy):
        return remote(halo.at[1], copy[0], halo_sems.at[4], copy[1], copy[2])

    wrap_r = to_both_tm((halo.at[0], halo_sems.at[1], {"tile": tile_r}))
    wrap_l = to_both_tm((halo.at[2], halo_sems.at[3], {"tile": tile_l}))
    sends_r = jnp.logical_not(high & tail)
    sends_l = jnp.logical_not(head & jnp.logical_not(odd))
    right_tile = {"tm": jnp.where(tail, tm_r, t), "tile": tile_r}

    @pl.when(sends_r)
    def _():
        to_right(right_tile).start()

    @pl.when(sends_l)
    def _():
        to_left(last_tile).start()

    @pl.when(low & tail)
    def _():
        wrap_r.start()

    @pl.when(odd & head)
    def _():
        wrap_l.start()

    @pl.when((t == 1) | (t == 2))
    def _():
        signal(ready_next, back)

    @pl.when(t >= 2)
    def _():
        signal(ready_back, onward)

    for load in loads[1:5]:
        load.wait()
    for w in range(windows):
        b = weight[w]
        later = slot_index[w] - 2 * t == 1
        scale[w, 0] = jnp.full((8, 128), jnp.where(later, 1.0, b), jnp.float32)
        scale[w, 1] = jnp.full((8, 128), jnp.where(later, b, 0.0), jnp.float32)

    @pl.when(t == 0)
    def _():
        def clear(i, carry):
            gath[i // nc, lax.rem(i, nc), 2] = jnp.zeros((lc, 8, 128), jnp.float32)
            return carry

        lax.fori_loop(0, n_mem * nc, clear, 0)

    fields = 2 * members
    groups = [(k // 8, min(8, fields - k)) for k in range(0, fields, 8)]
    with scope("own"):
        for group, rows in groups:
            smooth_own(halo, own, group, rows)
    with scope("halo"):
        to_right(next_tile).wait_recv()
        to_left(last_tile).wait_recv()

    with scope("smooth"):
        for group, rows in groups:
            smooth_rest(halo, own, f_ref, counts, norm, group, rows)
        loads[5].wait()

    def part(quarter, chunk, dst):
        def body(p, carry):
            lp = quarter * quarter_pairs + chunk * pairs + p
            v = [[modes[mode, 2 * lp + j] for mode in range(2)] for j in range(2)]
            acc = [[None, None], [None, None]]
            for k in range(members):
                f0 = f_ref[pl.ds(16 * k, 8), :]
                f1 = f_ref[pl.ds(16 * k + 8, 8), :]
                loc = [v[j][0] * f0 + v[j][1] * f1 for j in range(2)]
                for s in range(2):
                    x = pert[k, s, lp].astype(jnp.float32)
                    for j in range(2):
                        term = loc[j] * x[8 * j : 8 * j + 8]
                        acc[s][j] = term if k == 0 else acc[s][j] + term
            for s in range(2):
                for j in range(2):
                    dst[s, 2 * p + j] = acc[s][j]
            return carry

        if pairs == 1:
            body(0, 0)
        else:
            lax.fori_loop(0, pairs, body, 0)

    late = place >= run - 4

    half = nc // 2
    hops = nc * lc // HOP
    bases = (-DIRECT, nc - DIRECT, 2 * nc - DIRECT, 2 * nc - DIRECT + hops)
    bases += (bases[3] + half, bases[3] + half + 2, bases[3] + half + 3)
    bases += (bases[6] + 1,)
    shares = (1, 1, 1, 2, half, nc, nc, 2)

    def channel(k, c, src, dst, device):
        return remote(src, dst, send.at[k], recv.at[bases[k] + c // shares[k]], device)

    def arrive(k, c, size):
        channel(k, c, size, size, right).wait_recv()

    def sent(k, size):
        remote(size, size, send.at[k], recv.at[0], right).wait_send()

    def both(ref):
        return ref.at[pl.ds(0, 2)]

    def units(c):
        return [u for u in range(nc * lc // HOP) if c * lc < (u + 1) * HOP <= (c + 1) * lc]

    def chain(u):
        levels = pl.ds(u * HOP, HOP)
        return channel(2, u, za_out.at[levels], za_in.at[levels], onward)

    def around(c):
        two = pl.ds((c - 1) * lc, 2 * lc)
        return channel(3, c, za_out.at[two], zb_in.at[two], back)

    def relay(c):
        two = pl.ds((c - 1) * lc, 2 * lc)
        return channel(3, c, zb_in.at[two], zb_in.at[two], back)

    def bypass(c):
        two = pl.ds((c - 1) * lc, 2 * lc)
        return channel(7, c, zb_in.at[two], zc_in.at[two], back)

    direct = range(DIRECT)
    ringed = range(DIRECT, nc)

    def send_near(c, side):
        channel(1, c, near.at[c, side], mail.at[c, side], (right, left)[side]).start()

    with scope("far"):
        for c in ringed:
            part(mem_f, c, far.at[c])
            channel(0, c, far.at[c, 0], mail_far.at[c, 0], right).start()
            channel(0, c, far.at[c, 1], mail_far.at[c, 1], left).start()
        for c in direct:
            part(mem_f, c, far.at[c])
            remote(far.at[c], mail.at[c, 2], send.at[0], recv.at[bases[1] + c], across).start()
            part(mem_r, c, near.at[c, 0])
            send_near(c, 0)
            part(mem_l, c, near.at[c, 1])
            send_near(c, 1)
    with scope("near"):
        for c in ringed:
            part(mem_r, c, near.at[c, 0])
            part(mem_l, c, near.at[c, 1])
        for c in range(nc):
            part(m, c, gath.at[m, c])

    def step_a(c):
        arrive(0, c, mail_far.at[c])
        near[c, 0, 0] += mail_far[c, 0]
        send_near(c, 0)
        near[c, 1, 1] += mail_far[c, 1]
        send_near(c, 1)

    def step_b(c):
        sources = 3 if c < DIRECT else 2
        arrive(1, c, mail.at[c, pl.ds(0, sources)])
        for level in range(lc):
            total = None
            for s in range(2):
                value = mail[c, 0, s, level] + mail[c, 1, s, level]
                if sources == 3:
                    value = value + mail[c, 2, s, level]
                value = gath[m, c, s, level] + value
                gath[m, c, s, level] = value
                total = value if s == 0 else total + value
            za_out[c * lc + level] = total

        if c == 0:
            @pl.when(t < 2)
            def _():
                pl.semaphore_wait(ready_next, 1)

            @pl.when((t == 0) | (t == 3))
            def _():
                pl.semaphore_wait(ready_back, 1)

        @pl.when((t < 2) | (late & (t == 2)))
        def _():
            for u in units(c):
                chain(u).start()

        if c % 2 == 1:
            @pl.when((t == 0) | (late & (t == 1)))
            def _():
                around(c).start()

    def step_g(c):
        mine = both(gath.at[m, c])
        for device in (right, left):
            channel(4, c, mine, mine, device).start()
        if c >= half:
            remote(mine, mine, send.at[5], recv.at[bases[4] + 1], across).start()

    def step_z2(c):
        for u in units(c):
            chain(u).wait_recv()
            for level in range(u * HOP, (u + 1) * HOP):
                za_out[level] += za_in[level]
            chain(u).start()

    def step_z3(c):
        if c % 2 == 1:
            around(c).wait_recv()
            relay(c).start()

    def step_d():
        arrive(4, 0, near.at[pl.ds(0, half)])
        for c in range(half):
            channel(5, 0, gath.at[mem_l, c, 0], gath.at[mem_l, c, 0], right).start()
            channel(5, 0, gath.at[mem_r, c, 1], gath.at[mem_r, c, 1], left).start()

    def early_1(level):
        return za_in[level]

    def early_23(level):
        return za_in[level] + zb_in[level]

    def step_e(c, early):
        def come():
            for u in units(c):
                chain(u).wait_recv()

        if early is early_23 and c % 2 == 0:
            @pl.when(t == 2)
            def _():
                relay(c + 1).wait_recv()

            @pl.when(late & (t == 3))
            def _():
                bypass(c + 1).wait_recv()

        pl.when((t != 2) | late)(come)
        for level in range(lc):
            gath[m, c, 2, level] = early(c * lc + level)
        if early is early_23:
            @pl.when(late & (t == 3))
            def _():
                for level in range(lc):
                    gath[m, c, 2, level] += zc_in[c * lc + level]

        for device in (across, right, left):
            channel(6, c, gath.at[m, c, 2], gath.at[m, c, 2], device).start()

    def play(steps):
        for step, *args in steps:
            with scope(f"{step.__name__.replace("step_","").upper()[0]}{args[0]}"):
                step(*args)

    every = range(nc)
    first = [(step_a, c) for c in ringed[:1]]
    for k in range(max(DIRECT, nc - DIRECT - 1)):
        if DIRECT + 1 + k < nc:
            first.append((step_a, DIRECT + 1 + k))
        if k < DIRECT:
            first.append((step_b, k))
    play(first)

    def rest(also=None):
        for c in ringed:
            play([(step_b, c)])
            if also is not None:
                play([(also, c)])
            play([(step_g, k) for k in (range(DIRECT + 1) if c == DIRECT else (c,))])

    @pl.when(t == 0)
    def _():
        rest()
        step_d()

        @pl.when(late)
        def _():
            for c in range(1, nc, 2):
                around(c).wait_recv()
                bypass(c).start()

    @pl.when(t == 1)
    def _():
        play([(step_b, c) for c in ringed] + [(step_g, c) for c in every])
        play([(step_e, c, early_1) for c in range(half)])
        step_d()
        play([(step_e, c, early_1) for c in range(half, nc)])

    @pl.when((t == 2) & jnp.logical_not(late))
    def _():
        play([(step_z2, c) for c in direct])
        rest(step_z2)

    @pl.when((t == 2) & late)
    def _():
        rest()

    @pl.when(t == 2)
    def _():
        play([(step_e, c, early_23) for c in range(half)])
        step_d()
        play([(step_e, c, early_23) for c in range(half, nc)])

    @pl.when(t == 3)
    def _():
        play([(step_z3, c) for c in direct])
        rest(step_z3)
        step_d()
        play([(step_e, c, early_23) for c in every])

    with scope("P"):
        arrive(4, half, mail.at[pl.ds(0, half)])
        arrive(5, 0, far.at[pl.ds(0, half)])
    with scope("H"):
        @pl.when(t > 0)
        def _():
            arrive(6, 0, gath.at[0])

    with scope("W"):
        @pl.when(sends_r)
        def _():
            to_right(right_tile).wait_send()

        @pl.when(sends_l)
        def _():
            to_left(last_tile).wait_send()

        @pl.when((low & tail) | (odd & head))
        def _():
            wrap_r.wait_send()

        sent(0, far)
        sent(1, near)
        sent(4, near)
        sent(5, far)

        @pl.when(t < 3)
        def _():
            sent(2, za_out)

        @pl.when((t == 0) | (t == 3))
        def _():
            sent(3, za_out)

        @pl.when(late & (t == 1))
        def _():
            sent(3, za_out)

        @pl.when(late & (t == 0))
        def _():
            sent(7, za_out)

        @pl.when(t > 0)
        def _():
            sent(6, gath.at[0])


def blend_kernel(gath, scale, out, block, sems):
    n_mem, nc, _, lc = gath.shape[:4]
    windows = block.shape[0]
    copies = []
    for w in range(windows):
        a, b = scale[w, 0], scale[w, 1]
        for q in range(n_mem):
            for c in range(nc):
                for level in range(lc):
                    r0, r1, e = (gath[q, c, i, level] for i in range(3))
                    block[w, (q * nc + c) * lc + level] = e + (a * r0 + b * r1)
        copies.append(pltpu.make_async_copy(block.at[w], out.at[w], sems.at[w]))
        copies[-1].start()
    for copy in copies:
        copy.wait()


def solution(mesh):
    n_tm, n_mem, n_tile = (mesh.shape[a] for a in ("tm", "mem", "tile"))

    def folded(x):
        *lead, rows, columns = x.shape
        x = x.reshape(*lead, rows, columns // 128, 128)
        x = jnp.swapaxes(x, -3, -2)
        return x.reshape(*lead, rows * (columns // 128), 128)

    def per_device(control, vertical_modes, mode_counts, perturbations, slot_index, blend_weight):
        members, slots, levels = perturbations.shape[:3]
        windows = slot_index.shape[0]
        ctrl = folded(control).reshape(-1, 128)
        pert = folded(perturbations).reshape(members, slots, levels // 2, 16, 128)
        rows = ctrl.shape[0]
        nc = CHUNKS
        lc = levels // n_mem // nc
        f32 = jnp.float32
        slot = (nc, slots, lc, 8, 128)
        one = (nc * lc, 8, 128)
        vmem = pl.BlockSpec(memory_space=pltpu.VMEM)
        hbm = pl.BlockSpec(memory_space=pl.ANY)
        dma = pltpu.SemaphoreType.DMA
        regular = pltpu.SemaphoreType.REGULAR
        gath, scale = pl.pallas_call(
            functools.partial(kernel, n_tm, n_mem, n_tile, members, windows),
            out_shape=(
                pltpu.VMEM((n_mem, nc, 3, lc, 8, 128), f32),
                pltpu.VMEM((windows, 2, 8, 128), f32),
            ),
            in_specs=[hbm] * 6,
            out_specs=(vmem, vmem),
            scratch_shapes=[
                pltpu.VMEM((3, rows, 128), f32), pltpu.VMEM((8 * -(-2 * members // 8), 8, 128), f32),
                pltpu.VMEM(pert.shape, jnp.bfloat16),
                pltpu.VMEM((rows, 128), f32),
                pltpu.VMEM(slot, f32), pltpu.VMEM((nc, 2, *slot[1:]), f32),
                pltpu.VMEM(slot, f32), pltpu.VMEM((nc, 3, *slot[1:]), f32),
                pltpu.VMEM(one, f32), pltpu.VMEM(one, f32), pltpu.VMEM(one, f32), pltpu.VMEM(one, f32),
                pltpu.SMEM((2, levels), f32), pltpu.SMEM(mode_counts.shape, jnp.int32),
                pltpu.SMEM((windows,), jnp.int32), pltpu.SMEM((windows,), f32),
                dma((5,)), dma((8,)), dma((2 * nc - DIRECT + nc * lc // HOP + nc + 4,)), regular, regular,
            ],
            compiler_params=pltpu.CompilerParams(collective_id=0, has_side_effects=True),
        )(ctrl, pert, vertical_modes.T, mode_counts, slot_index, blend_weight)
        out = pl.pallas_call(
            blend_kernel,
            out_shape=jax.ShapeDtypeStruct((windows, levels, 8, 128), f32),
            in_specs=[vmem, vmem],
            out_specs=hbm,
            scratch_shapes=[pltpu.VMEM((windows, levels, 8, 128), f32), dma((windows,))],
        )(*(pltpu.with_memory_space_constraint(x, pltpu.VMEM) for x in (gath, scale)))
        out = out.reshape(windows, levels, 2, 4, 128)
        return jnp.swapaxes(out, -3, -2).reshape(windows, levels, 4, 256)

    return jax.shard_map(
        per_device,
        mesh=mesh,
        in_specs=(
            P("mem", None, "tile", None), P(), P("tile"),
            P("mem", "tm", None, "tile", None), P("tm"), P("tm"),
        ),
        out_specs=P("tm", None, "tile", None),
        check_vma=False,
    )
```

```python
import functools
import math
from contextlib import nullcontext as scope

import jax
import jax.numpy as jnp
from jax import lax
from jax.experimental import pallas as pl
from jax.experimental.pallas import tpu as pltpu
from jax.sharding import PartitionSpec as P

SMOOTH = 4
DIFFUSION = 0.24
CHUNKS = 8
HOP = 2
DIRECT = 4
MESH = pl.DeviceIdType.MESH


def spread():
    a, b = 1.0 - 4.0 * DIFFUSION, DIFFUSION
    weights = [[0.0] * (SMOOTH - d + 1) for d in range(SMOOTH + 1)]
    for k in range(SMOOTH + 1):
        for d in range(k % 2, k + 1, 2):
            outer = math.comb(SMOOTH, k) * b**k * math.comb(k, (k - d) // 2)
            for j in range(SMOOTH - k + 1):
                weights[d][j] += outer * math.comb(SMOOTH - k, j) * a ** (SMOOTH - k - j) * b**j
    return weights


def add_rows(halo, total, group, rows, longitudes):
    weights = spread()
    lane = lax.broadcasted_iota(jnp.int32, (rows, 128), 1)
    first, last = lane == 0, lane == 127
    for x in longitudes:
        tile, inner = (x + 4) // 4, x % 4
        reach = [(r, abs(r - x)) for r in range(4) if abs(r - x) <= SMOOTH]
        pair = [halo[tile, pl.ds(group * 64 + h * 4 + inner, rows, 8), :] for h in range(2)]
        for j in range(SMOOTH - min(d for _, d in reach) + 1):
            if j:
                up = [pltpu.roll(v, 1, 1) for v in pair]
                down = [pltpu.roll(v, 127, 1) for v in pair]
                pair = [
                    jnp.where(first, 0.0, up[0]) + jnp.where(last, down[1], down[0]),
                    jnp.where(first, up[0], up[1]) + jnp.where(last, 0.0, down[1]),
                ]
            for r, d in reach:
                if j <= SMOOTH - d:
                    for h in range(2):
                        term = weights[d][j] * pair[h]
                        total[r, h] = total[r, h] + term if (r, h) in total else term


def smooth_own(halo, own, group, rows):
    total = {}
    add_rows(halo, total, group, rows, range(4))
    for (x, h), value in total.items():
        own[group * 8 + h * 4 + x, pl.ds(0, rows)] = value


def smooth_rest(halo, own, f_ref, counts, norm, group, rows):
    total = {
        (x, h): own[group * 8 + h * 4 + x, pl.ds(0, rows)] for x in range(4) for h in range(2)
    }
    add_rows(halo, total, group, rows, (-4, -3, -2, -1, 4, 5, 6, 7))
    mode = lax.broadcasted_iota(jnp.int32, (rows, 128), 0) % 2
    for x in range(4):
        scales = [jnp.where(m < counts[x], norm, 0.0) for m in range(2)]
        scale = jnp.where(mode == 0, scales[0], scales[1])
        for h in range(2):
            f_ref[pl.ds(group * 64 + h * 4 + x, rows, 8), :] = total[x, h] * scale


def kernel(
    n_tm, n_mem, n_tile, members, windows,
    ctrl, pert_hbm, modes_hbm, counts_hbm, index_hbm, weight_hbm,
    gath, scale,
    halo, own, pert, f_ref, far, near, mail_far, mail,
    za_out, za_in, zb_in, zc_in, modes, counts, slot_index, weight,
    halo_sems, send, recv, ready_next, ready_back,
):
    t, m = lax.axis_index("tm"), lax.axis_index("mem")
    tile = lax.axis_index("tile")
    nc = far.shape[0]
    lc = far.shape[2]
    pairs = lc // 2
    quarter_pairs = nc * pairs
    norm = 1.0 / math.sqrt(members * n_mem - 1)

    mem_r, mem_l = lax.rem(m + 1, n_mem), lax.rem(m + n_mem - 1, n_mem)
    mem_f = lax.rem(m + 2, n_mem)
    tm_r, tm_l = lax.rem(t + 1, n_tm), lax.rem(t + n_tm - 1, n_tm)
    right, left, across = {"mem": mem_r}, {"mem": mem_l}, {"mem": mem_f}
    onward, back = {"tm": tm_r}, {"tm": tm_l}
    run = n_tile // 4
    place = lax.rem(tile, run)
    tile_r, tile_l = lax.rem(tile + 1, n_tile), lax.rem(tile + n_tile - 1, n_tile)
    head, tail = place == 0, place == run - 1
    low, high, odd = t == 0, t == n_tm - 1, lax.rem(t, 2) == 1
    step_r = jnp.where(tail & jnp.logical_not(odd), tm_r, t)
    step_l = jnp.where(head & jnp.logical_not(low), tm_l, t)
    next_tile = {"tm": step_r, "tile": tile_r}
    last_tile = {"tm": step_l, "tile": tile_l}

    def signal(sem, device):
        pl.semaphore_signal(sem, inc=1, device_id=device, device_id_type=MESH)

    barrier = pltpu.get_barrier_semaphore()
    partners = (next_tile, last_tile, right, left, across)
    for partner in partners:
        signal(barrier, partner)

    @pl.when(t < 2)
    def _():
        signal(barrier, onward)

    @pl.when((t == 0) | (t == 3))
    def _():
        signal(barrier, back)

    loads = [
        pltpu.make_async_copy(src, dst, send.at[k])
        for k, (src, dst) in enumerate((
            (ctrl, halo.at[1]), (counts_hbm, counts), (modes_hbm, modes),
            (index_hbm, slot_index), (weight_hbm, weight), (pert_hbm, pert),
        ))
    ]
    for load in loads:
        load.start()
    with scope("barrier"):
        loads[0].wait()
        extra = jnp.where(t == 0, 0, jnp.where(t == 2, 2, 1))
        extra += jnp.where((low & tail) | (odd & head), 1, 0)
        extra -= jnp.where((jnp.logical_not(odd) & head) | (high & tail), 1, 0)
        pl.semaphore_wait(barrier, len(partners) + extra)

    def remote(src, dst, s, r, device):
        return pltpu.make_async_remote_copy(
            src_ref=src, dst_ref=dst, send_sem=s, recv_sem=r,
            device_id=device, device_id_type=MESH,
        )

    def to_right(device):
        return remote(halo.at[1], halo.at[0], halo_sems.at[0], halo_sems.at[1], device)

    def to_left(device):
        return remote(halo.at[1], halo.at[2], halo_sems.at[2], halo_sems.at[3], device)

    def to_both_tm(copy):
        return remote(halo.at[1], copy[0], halo_sems.at[4], copy[1], copy[2])

    wrap_r = to_both_tm((halo.at[0], halo_sems.at[1], {"tile": tile_r}))
    wrap_l = to_both_tm((halo.at[2], halo_sems.at[3], {"tile": tile_l}))
    sends_r = jnp.logical_not(high & tail)
    sends_l = jnp.logical_not(head & jnp.logical_not(odd))
    right_tile = {"tm": jnp.where(tail, tm_r, t), "tile": tile_r}

    @pl.when(sends_r)
    def _():
        to_right(right_tile).start()

    @pl.when(sends_l)
    def _():
        to_left(last_tile).start()

    @pl.when(low & tail)
    def _():
        wrap_r.start()

    @pl.when(odd & head)
    def _():
        wrap_l.start()

    @pl.when((t == 1) | (t == 2))
    def _():
        signal(ready_next, back)

    @pl.when(t >= 2)
    def _():
        signal(ready_back, onward)

    for load in loads[1:5]:
        load.wait()
    for w in range(windows):
        b = weight[w]
        later = slot_index[w] - 2 * t == 1
        scale[w, 0] = jnp.full((8, 128), jnp.where(later, 1.0, b), jnp.float32)
        scale[w, 1] = jnp.full((8, 128), jnp.where(later, b, 0.0), jnp.float32)

    @pl.when(t == 0)
    def _():
        def clear(i, carry):
            gath[i // nc, lax.rem(i, nc), 2] = jnp.zeros((lc, 8, 128), jnp.float32)
            return carry

        lax.fori_loop(0, n_mem * nc, clear, 0)

    fields = 2 * members
    groups = [(k // 8, min(8, fields - k)) for k in range(0, fields, 8)]
    with scope("own"):
        for group, rows in groups:
            smooth_own(halo, own, group, rows)
    with scope("halo"):
        to_right(next_tile).wait_recv()
        to_left(last_tile).wait_recv()

    with scope("smooth"):
        for group, rows in groups:
            smooth_rest(halo, own, f_ref, counts, norm, group, rows)
        loads[5].wait()

    def part(quarter, chunk, dst):
        def body(p, carry):
            lp = quarter * quarter_pairs + chunk * pairs + p
            v = [[modes[mode, 2 * lp + j] for mode in range(2)] for j in range(2)]
            acc = [[None, None], [None, None]]
            for k in range(members):
                f0 = f_ref[pl.ds(16 * k, 8), :]
                f1 = f_ref[pl.ds(16 * k + 8, 8), :]
                loc = [v[j][0] * f0 + v[j][1] * f1 for j in range(2)]
                for s in range(2):
                    x = pert[k, s, lp].astype(jnp.float32)
                    for j in range(2):
                        term = loc[j] * x[8 * j : 8 * j + 8]
                        acc[s][j] = term if k == 0 else acc[s][j] + term
            for s in range(2):
                for j in range(2):
                    dst[s, 2 * p + j] = acc[s][j]
            return carry

        if pairs == 1:
            body(0, 0)
        else:
            lax.fori_loop(0, pairs, body, 0)

    late = place >= run - 4

    half = nc // 2
    hops = nc * lc // HOP
    bases = (-DIRECT, nc - DIRECT, 2 * nc - DIRECT, 2 * nc - DIRECT + hops)
    bases += (bases[3] + half, bases[3] + half + 2, bases[3] + half + 3)
    bases += (bases[6] + 1,)
    shares = (1, 1, 1, 2, half, nc, nc, 2)

    def channel(k, c, src, dst, device):
        return remote(src, dst, send.at[k], recv.at[bases[k] + c // shares[k]], device)

    def arrive(k, c, size):
        channel(k, c, size, size, right).wait_recv()

    def sent(k, size):
        remote(size, size, send.at[k], recv.at[0], right).wait_send()

    def both(ref):
        return ref.at[pl.ds(0, 2)]

    def units(c):
        return [u for u in range(nc * lc // HOP) if c * lc < (u + 1) * HOP <= (c + 1) * lc]

    def chain(u):
        levels = pl.ds(u * HOP, HOP)
        return channel(2, u, za_out.at[levels], za_in.at[levels], onward)

    def around(c):
        two = pl.ds((c - 1) * lc, 2 * lc)
        return channel(3, c, za_out.at[two], zb_in.at[two], back)

    def relay(c):
        two = pl.ds((c - 1) * lc, 2 * lc)
        return channel(3, c, zb_in.at[two], zb_in.at[two], back)

    def bypass(c):
        two = pl.ds((c - 1) * lc, 2 * lc)
        return channel(7, c, zb_in.at[two], zc_in.at[two], back)

    direct = range(DIRECT)
    ringed = range(DIRECT, nc)

    def send_near(c, side):
        channel(1, c, near.at[c, side], mail.at[c, side], (right, left)[side]).start()

    with scope("far"):
        for c in ringed:
            part(mem_f, c, far.at[c])
            channel(0, c, far.at[c, 0], mail_far.at[c, 0], right).start()
            channel(0, c, far.at[c, 1], mail_far.at[c, 1], left).start()
        for c in direct:
            part(mem_f, c, far.at[c])
            remote(far.at[c], mail.at[c, 2], send.at[0], recv.at[bases[1] + c], across).start()
            part(mem_r, c, near.at[c, 0])
            send_near(c, 0)
            part(mem_l, c, near.at[c, 1])
            send_near(c, 1)
    with scope("near"):
        for c in ringed:
            part(mem_r, c, near.at[c, 0])
            part(mem_l, c, near.at[c, 1])
        for c in range(nc):
            part(m, c, gath.at[m, c])

    def step_a(c):
        arrive(0, c, mail_far.at[c])
        near[c, 0, 0] += mail_far[c, 0]
        send_near(c, 0)
        near[c, 1, 1] += mail_far[c, 1]
        send_near(c, 1)

    def step_b(c):
        sources = 3 if c < DIRECT else 2
        arrive(1, c, mail.at[c, pl.ds(0, sources)])
        for level in range(lc):
            total = None
            for s in range(2):
                value = mail[c, 0, s, level] + mail[c, 1, s, level]
                if sources == 3:
                    value = value + mail[c, 2, s, level]
                value = gath[m, c, s, level] + value
                gath[m, c, s, level] = value
                total = value if s == 0 else total + value
            za_out[c * lc + level] = total

        if c == 0:
            @pl.when(t < 2)
            def _():
                pl.semaphore_wait(ready_next, 1)

            @pl.when((t == 0) | (t == 3))
            def _():
                pl.semaphore_wait(ready_back, 1)

        @pl.when((t < 2) | (late & (t == 2)))
        def _():
            for u in units(c):
                chain(u).start()

        if c % 2 == 1:
            @pl.when((t == 0) | (late & (t == 1)))
            def _():
                around(c).start()

    def step_g(c):
        mine = both(gath.at[m, c])
        for device in (right, left):
            channel(4, c, mine, mine, device).start()
        if c >= half:
            remote(mine, mine, send.at[5], recv.at[bases[4] + 1], across).start()

    def step_z2(c):
        for u in units(c):
            chain(u).wait_recv()
            for level in range(u * HOP, (u + 1) * HOP):
                za_out[level] += za_in[level]
            chain(u).start()

    def step_z3(c):
        if c % 2 == 1:
            around(c).wait_recv()
            relay(c).start()

    def step_d():
        arrive(4, 0, near.at[pl.ds(0, half)])
        for c in range(half):
            channel(5, 0, gath.at[mem_l, c, 0], gath.at[mem_l, c, 0], right).start()
            channel(5, 0, gath.at[mem_r, c, 1], gath.at[mem_r, c, 1], left).start()

    def early_1(level):
        return za_in[level]

    def early_23(level):
        return za_in[level] + zb_in[level]

    def step_e(c, early):
        def come():
            for u in units(c):
                chain(u).wait_recv()

        if early is early_23 and c % 2 == 0:
            @pl.when(t == 2)
            def _():
                relay(c + 1).wait_recv()

            @pl.when(late & (t == 3))
            def _():
                bypass(c + 1).wait_recv()

        pl.when((t != 2) | late)(come)
        for level in range(lc):
            gath[m, c, 2, level] = early(c * lc + level)
        if early is early_23:
            @pl.when(late & (t == 3))
            def _():
                for level in range(lc):
                    gath[m, c, 2, level] += zc_in[c * lc + level]

        for device in (across, right, left):
            channel(6, c, gath.at[m, c, 2], gath.at[m, c, 2], device).start()

    def play(steps):
        for step, *args in steps:
            with scope(f"{step.__name__.replace("step_","").upper()[0]}{args[0]}"):
                step(*args)

    every = range(nc)
    first = [(step_a, c) for c in ringed[:1]]
    for k in range(max(DIRECT, nc - DIRECT - 1)):
        if DIRECT + 1 + k < nc:
            first.append((step_a, DIRECT + 1 + k))
        if k < DIRECT:
            first.append((step_b, k))
    play(first)

    def rest(also=None):
        for c in ringed:
            play([(step_b, c)])
            if also is not None:
                play([(also, c)])
            play([(step_g, k) for k in (range(DIRECT + 1) if c == DIRECT else (c,))])

    @pl.when(t == 0)
    def _():
        rest()
        step_d()

        @pl.when(late)
        def _():
            for c in range(1, nc, 2):
                around(c).wait_recv()
                bypass(c).start()

    @pl.when(t == 1)
    def _():
        play([(step_b, c) for c in ringed] + [(step_g, c) for c in every])
        play([(step_e, c, early_1) for c in range(half)])
        step_d()
        play([(step_e, c, early_1) for c in range(half, nc)])

    @pl.when((t == 2) & jnp.logical_not(late))
    def _():
        play([(step_z2, c) for c in direct])
        rest(step_z2)

    @pl.when((t == 2) & late)
    def _():
        rest()

    @pl.when(t == 2)
    def _():
        play([(step_e, c, early_23) for c in range(half)])
        step_d()
        play([(step_e, c, early_23) for c in range(half, nc)])

    @pl.when(t == 3)
    def _():
        play([(step_z3, c) for c in direct])
        rest(step_z3)
        step_d()
        play([(step_e, c, early_23) for c in every])

    with scope("P"):
        arrive(4, half, mail.at[pl.ds(0, half)])
        arrive(5, 0, far.at[pl.ds(0, half)])
    with scope("H"):
        @pl.when(t > 0)
        def _():
            arrive(6, 0, gath.at[0])

    with scope("W"):
        @pl.when(sends_r)
        def _():
            to_right(right_tile).wait_send()

        @pl.when(sends_l)
        def _():
            to_left(last_tile).wait_send()

        @pl.when((low & tail) | (odd & head))
        def _():
            wrap_r.wait_send()

        sent(0, far)
        sent(1, near)
        sent(4, near)
        sent(5, far)

        @pl.when(t < 3)
        def _():
            sent(2, za_out)

        @pl.when((t == 0) | (t == 3))
        def _():
            sent(3, za_out)

        @pl.when(late & (t == 1))
        def _():
            sent(3, za_out)

        @pl.when(late & (t == 0))
        def _():
            sent(7, za_out)

        @pl.when(t > 0)
        def _():
            sent(6, gath.at[0])


def blend_kernel(gath, scale, out, block, sems):
    n_mem, nc, _, lc = gath.shape[:4]
    windows = block.shape[0]
    copies = []
    for w in range(windows):
        a, b = scale[w, 0], scale[w, 1]
        for q in range(n_mem):
            for c in range(nc):
                for level in range(lc):
                    r0, r1, e = (gath[q, c, i, level] for i in range(3))
                    block[w, (q * nc + c) * lc + level] = e + (a * r0 + b * r1)
        copies.append(pltpu.make_async_copy(block.at[w], out.at[w], sems.at[w]))
        copies[-1].start()
    for copy in copies:
        copy.wait()


def solution(mesh):
    n_tm, n_mem, n_tile = (mesh.shape[a] for a in ("tm", "mem", "tile"))

    def folded(x):
        *lead, rows, columns = x.shape
        x = x.reshape(*lead, rows, columns // 128, 128)
        x = jnp.swapaxes(x, -3, -2)
        return x.reshape(*lead, rows * (columns // 128), 128)

    def per_device(control, vertical_modes, mode_counts, perturbations, slot_index, blend_weight):
        members, slots, levels = perturbations.shape[:3]
        windows = slot_index.shape[0]
        ctrl = folded(control).reshape(-1, 128)
        pert = folded(perturbations).reshape(members, slots, levels // 2, 16, 128)
        rows = ctrl.shape[0]
        nc = CHUNKS
        lc = levels // n_mem // nc
        f32 = jnp.float32
        slot = (nc, slots, lc, 8, 128)
        one = (nc * lc, 8, 128)
        vmem = pl.BlockSpec(memory_space=pltpu.VMEM)
        hbm = pl.BlockSpec(memory_space=pl.ANY)
        dma = pltpu.SemaphoreType.DMA
        regular = pltpu.SemaphoreType.REGULAR
        gath, scale = pl.pallas_call(
            functools.partial(kernel, n_tm, n_mem, n_tile, members, windows),
            out_shape=(
                pltpu.VMEM((n_mem, nc, 3, lc, 8, 128), f32),
                pltpu.VMEM((windows, 2, 8, 128), f32),
            ),
            in_specs=[hbm] * 6,
            out_specs=(vmem, vmem),
            scratch_shapes=[
                pltpu.VMEM((3, rows, 128), f32), pltpu.VMEM((8 * -(-2 * members // 8), 8, 128), f32),
                pltpu.VMEM(pert.shape, jnp.bfloat16),
                pltpu.VMEM((rows, 128), f32),
                pltpu.VMEM(slot, f32), pltpu.VMEM((nc, 2, *slot[1:]), f32),
                pltpu.VMEM(slot, f32), pltpu.VMEM((nc, 3, *slot[1:]), f32),
                pltpu.VMEM(one, f32), pltpu.VMEM(one, f32), pltpu.VMEM(one, f32), pltpu.VMEM(one, f32),
                pltpu.SMEM((2, levels), f32), pltpu.SMEM(mode_counts.shape, jnp.int32),
                pltpu.SMEM((windows,), jnp.int32), pltpu.SMEM((windows,), f32),
                dma((5,)), dma((8,)), dma((2 * nc - DIRECT + nc * lc // HOP + nc + 4,)), regular, regular,
            ],
            compiler_params=pltpu.CompilerParams(collective_id=0, has_side_effects=True),
        )(ctrl, pert, vertical_modes.T, mode_counts, slot_index, blend_weight)
        out = pl.pallas_call(
            blend_kernel,
            out_shape=jax.ShapeDtypeStruct((windows, levels, 8, 128), f32),
            in_specs=[vmem, vmem],
            out_specs=hbm,
            scratch_shapes=[pltpu.VMEM((windows, levels, 8, 128), f32), dma((windows,))],
        )(*(pltpu.with_memory_space_constraint(x, pltpu.VMEM) for x in (gath, scale)))
        out = out.reshape(windows, levels, 2, 4, 128)
        return jnp.swapaxes(out, -3, -2).reshape(windows, levels, 4, 256)

    return jax.shard_map(
        per_device,
        mesh=mesh,
        in_specs=(
            P("mem", None, "tile", None), P(), P("tile"),
            P("mem", "tm", None, "tile", None), P("tm"), P("tm"),
        ),
        out_specs=P("tm", None, "tile", None),
        check_vma=False,
    )
```

```python
import functools
import math
from contextlib import nullcontext as scope

import jax
import jax.numpy as jnp
from jax import lax
from jax.experimental import pallas as pl
from jax.experimental.pallas import tpu as pltpu
from jax.sharding import PartitionSpec as P

SMOOTH = 4
DIFFUSION = 0.24
CHUNKS = 8
HOP = 2
DIRECT = 4
MESH = pl.DeviceIdType.MESH


def spread():
    a, b = 1.0 - 4.0 * DIFFUSION, DIFFUSION
    weights = [[0.0] * (SMOOTH - d + 1) for d in range(SMOOTH + 1)]
    for k in range(SMOOTH + 1):
        for d in range(k % 2, k + 1, 2):
            outer = math.comb(SMOOTH, k) * b**k * math.comb(k, (k - d) // 2)
            for j in range(SMOOTH - k + 1):
                weights[d][j] += outer * math.comb(SMOOTH - k, j) * a ** (SMOOTH - k - j) * b**j
    return weights


def add_rows(halo, total, group, rows, longitudes):
    weights = spread()
    lane = lax.broadcasted_iota(jnp.int32, (rows, 128), 1)
    first, last = lane == 0, lane == 127
    for x in longitudes:
        tile, inner = (x + 4) // 4, x % 4
        reach = [(r, abs(r - x)) for r in range(4) if abs(r - x) <= SMOOTH]
        pair = [halo[tile, pl.ds(group * 64 + h * 4 + inner, rows, 8), :] for h in range(2)]
        for j in range(SMOOTH - min(d for _, d in reach) + 1):
            if j:
                up = [pltpu.roll(v, 1, 1) for v in pair]
                down = [pltpu.roll(v, 127, 1) for v in pair]
                pair = [
                    jnp.where(first, 0.0, up[0]) + jnp.where(last, down[1], down[0]),
                    jnp.where(first, up[0], up[1]) + jnp.where(last, 0.0, down[1]),
                ]
            for r, d in reach:
                if j <= SMOOTH - d:
                    for h in range(2):
                        term = weights[d][j] * pair[h]
                        total[r, h] = total[r, h] + term if (r, h) in total else term


def smooth_own(halo, own, group, rows):
    total = {}
    add_rows(halo, total, group, rows, range(4))
    for (x, h), value in total.items():
        own[group * 8 + h * 4 + x, pl.ds(0, rows)] = value


def smooth_rest(halo, own, f_ref, counts, norm, group, rows):
    total = {
        (x, h): own[group * 8 + h * 4 + x, pl.ds(0, rows)] for x in range(4) for h in range(2)
    }
    add_rows(halo, total, group, rows, (-4, -3, -2, -1, 4, 5, 6, 7))
    mode = lax.broadcasted_iota(jnp.int32, (rows, 128), 0) % 2
    for x in range(4):
        scales = [jnp.where(m < counts[x], norm, 0.0) for m in range(2)]
        scale = jnp.where(mode == 0, scales[0], scales[1])
        for h in range(2):
            f_ref[pl.ds(group * 64 + h * 4 + x, rows, 8), :] = total[x, h] * scale


def kernel(
    n_tm, n_mem, n_tile, members, windows,
    ctrl, pert_hbm, modes_hbm, counts_hbm, index_hbm, weight_hbm,
    gath, scale,
    halo, own, pert, f_ref, far, near, mail_far, mail,
    za_out, za_in, zb_in, zc_in, modes, counts, slot_index, weight,
    halo_sems, send, recv, ready_next, ready_back,
):
    t, m = lax.axis_index("tm"), lax.axis_index("mem")
    tile = lax.axis_index("tile")
    nc = far.shape[0]
    lc = far.shape[2]
    pairs = lc // 2
    quarter_pairs = nc * pairs
    norm = 1.0 / math.sqrt(members * n_mem - 1)

    mem_r, mem_l = lax.rem(m + 1, n_mem), lax.rem(m + n_mem - 1, n_mem)
    mem_f = lax.rem(m + 2, n_mem)
    tm_r, tm_l = lax.rem(t + 1, n_tm), lax.rem(t + n_tm - 1, n_tm)
    right, left, across = {"mem": mem_r}, {"mem": mem_l}, {"mem": mem_f}
    onward, back = {"tm": tm_r}, {"tm": tm_l}
    run = n_tile // 4
    place = lax.rem(tile, run)
    tile_r, tile_l = lax.rem(tile + 1, n_tile), lax.rem(tile + n_tile - 1, n_tile)
    head, tail = place == 0, place == run - 1
    low, high, odd = t == 0, t == n_tm - 1, lax.rem(t, 2) == 1
    step_r = jnp.where(tail & jnp.logical_not(odd), tm_r, t)
    step_l = jnp.where(head & jnp.logical_not(low), tm_l, t)
    next_tile = {"tm": step_r, "tile": tile_r}
    last_tile = {"tm": step_l, "tile": tile_l}

    def signal(sem, device):
        pl.semaphore_signal(sem, inc=1, device_id=device, device_id_type=MESH)

    barrier = pltpu.get_barrier_semaphore()
    partners = (next_tile, last_tile, right, left, across)
    for partner in partners:
        signal(barrier, partner)

    @pl.when(t < 2)
    def _():
        signal(barrier, onward)

    @pl.when((t == 0) | (t == 3))
    def _():
        signal(barrier, back)

    loads = [
        pltpu.make_async_copy(src, dst, send.at[k])
        for k, (src, dst) in enumerate((
            (ctrl, halo.at[1]), (counts_hbm, counts), (modes_hbm, modes),
            (index_hbm, slot_index), (weight_hbm, weight), (pert_hbm, pert),
        ))
    ]
    for load in loads:
        load.start()
    with scope("barrier"):
        loads[0].wait()
        extra = jnp.where(t == 0, 0, jnp.where(t == 2, 2, 1))
        extra += jnp.where((low & tail) | (odd & head), 1, 0)
        extra -= jnp.where((jnp.logical_not(odd) & head) | (high & tail), 1, 0)
        pl.semaphore_wait(barrier, len(partners) + extra)

    def remote(src, dst, s, r, device):
        return pltpu.make_async_remote_copy(
            src_ref=src, dst_ref=dst, send_sem=s, recv_sem=r,
            device_id=device, device_id_type=MESH,
        )

    def to_right(device):
        return remote(halo.at[1], halo.at[0], halo_sems.at[0], halo_sems.at[1], device)

    def to_left(device):
        return remote(halo.at[1], halo.at[2], halo_sems.at[2], halo_sems.at[3], device)

    def to_both_tm(copy):
        return remote(halo.at[1], copy[0], halo_sems.at[4], copy[1], copy[2])

    wrap_r = to_both_tm((halo.at[0], halo_sems.at[1], {"tile": tile_r}))
    wrap_l = to_both_tm((halo.at[2], halo_sems.at[3], {"tile": tile_l}))
    sends_r = jnp.logical_not(high & tail)
    sends_l = jnp.logical_not(head & jnp.logical_not(odd))
    right_tile = {"tm": jnp.where(tail, tm_r, t), "tile": tile_r}

    @pl.when(sends_r)
    def _():
        to_right(right_tile).start()

    @pl.when(sends_l)
    def _():
        to_left(last_tile).start()

    @pl.when(low & tail)
    def _():
        wrap_r.start()

    @pl.when(odd & head)
    def _():
        wrap_l.start()

    @pl.when((t == 1) | (t == 2))
    def _():
        signal(ready_next, back)

    @pl.when(t >= 2)
    def _():
        signal(ready_back, onward)

    for load in loads[1:5]:
        load.wait()
    for w in range(windows):
        b = weight[w]
        later = slot_index[w] - 2 * t == 1
        scale[w, 0] = jnp.full((8, 128), jnp.where(later, 1.0, b), jnp.float32)
        scale[w, 1] = jnp.full((8, 128), jnp.where(later, b, 0.0), jnp.float32)

    @pl.when(t == 0)
    def _():
        def clear(i, carry):
            gath[i // nc, lax.rem(i, nc), 2] = jnp.zeros((lc, 8, 128), jnp.float32)
            return carry

        lax.fori_loop(0, n_mem * nc, clear, 0)

    fields = 2 * members
    groups = [(k // 8, min(8, fields - k)) for k in range(0, fields, 8)]
    with scope("own"):
        for group, rows in groups:
            smooth_own(halo, own, group, rows)
    with scope("halo"):
        to_right(next_tile).wait_recv()
        to_left(last_tile).wait_recv()

    with scope("smooth"):
        for group, rows in groups:
            smooth_rest(halo, own, f_ref, counts, norm, group, rows)
        loads[5].wait()

    def part(quarter, chunk, dst):
        def body(p, carry):
            lp = quarter * quarter_pairs + chunk * pairs + p
            v = [[modes[mode, 2 * lp + j] for mode in range(2)] for j in range(2)]
            acc = [[None, None], [None, None]]
            for k in range(members):
                f0 = f_ref[pl.ds(16 * k, 8), :]
                f1 = f_ref[pl.ds(16 * k + 8, 8), :]
                loc = [v[j][0] * f0 + v[j][1] * f1 for j in range(2)]
                for s in range(2):
                    x = pert[k, s, lp].astype(jnp.float32)
                    for j in range(2):
                        term = loc[j] * x[8 * j : 8 * j + 8]
                        acc[s][j] = term if k == 0 else acc[s][j] + term
            for s in range(2):
                for j in range(2):
                    dst[s, 2 * p + j] = acc[s][j]
            return carry

        if pairs == 1:
            body(0, 0)
        else:
            lax.fori_loop(0, pairs, body, 0)

    late = place >= run - 4

    half = nc // 2
    hops = nc * lc // HOP
    bases = (-DIRECT, nc - DIRECT, 2 * nc - DIRECT, 2 * nc - DIRECT + hops)
    bases += (bases[3] + half, bases[3] + half + 2, bases[3] + half + 3)
    bases += (bases[6] + 1,)
    shares = (1, 1, 1, 2, half, nc, nc, 2)

    def channel(k, c, src, dst, device):
        return remote(src, dst, send.at[k], recv.at[bases[k] + c // shares[k]], device)

    def arrive(k, c, size):
        channel(k, c, size, size, right).wait_recv()

    def sent(k, size):
        remote(size, size, send.at[k], recv.at[0], right).wait_send()

    def both(ref):
        return ref.at[pl.ds(0, 2)]

    def units(c):
        return [u for u in range(nc * lc // HOP) if c * lc < (u + 1) * HOP <= (c + 1) * lc]

    def chain(u):
        levels = pl.ds(u * HOP, HOP)
        return channel(2, u, za_out.at[levels], za_in.at[levels], onward)

    def around(c):
        two = pl.ds((c - 1) * lc, 2 * lc)
        return channel(3, c, za_out.at[two], zb_in.at[two], back)

    def relay(c):
        two = pl.ds((c - 1) * lc, 2 * lc)
        return channel(3, c, zb_in.at[two], zb_in.at[two], back)

    def bypass(c):
        two = pl.ds((c - 1) * lc, 2 * lc)
        return channel(7, c, zb_in.at[two], zc_in.at[two], back)

    direct = range(DIRECT)
    ringed = range(DIRECT, nc)

    def send_near(c, side):
        channel(1, c, near.at[c, side], mail.at[c, side], (right, left)[side]).start()

    with scope("far"):
        for c in ringed:
            part(mem_f, c, far.at[c])
            channel(0, c, far.at[c, 0], mail_far.at[c, 0], right).start()
            channel(0, c, far.at[c, 1], mail_far.at[c, 1], left).start()
        for c in direct:
            part(mem_f, c, far.at[c])
            remote(far.at[c], mail.at[c, 2], send.at[0], recv.at[bases[1] + c], across).start()
            part(mem_r, c, near.at[c, 0])
            send_near(c, 0)
            part(mem_l, c, near.at[c, 1])
            send_near(c, 1)
    with scope("near"):
        for c in ringed:
            part(mem_r, c, near.at[c, 0])
            part(mem_l, c, near.at[c, 1])
        for c in range(nc):
            part(m, c, gath.at[m, c])

    def step_a(c):
        arrive(0, c, mail_far.at[c])
        near[c, 0, 0] += mail_far[c, 0]
        send_near(c, 0)
        near[c, 1, 1] += mail_far[c, 1]
        send_near(c, 1)

    def step_b(c):
        sources = 3 if c < DIRECT else 2
        arrive(1, c, mail.at[c, pl.ds(0, sources)])
        for level in range(lc):
            total = None
            for s in range(2):
                value = mail[c, 0, s, level] + mail[c, 1, s, level]
                if sources == 3:
                    value = value + mail[c, 2, s, level]
                value = gath[m, c, s, level] + value
                gath[m, c, s, level] = value
                total = value if s == 0 else total + value
            za_out[c * lc + level] = total

        if c == 0:
            @pl.when(t < 2)
            def _():
                pl.semaphore_wait(ready_next, 1)

            @pl.when((t == 0) | (t == 3))
            def _():
                pl.semaphore_wait(ready_back, 1)

        @pl.when((t < 2) | (late & (t == 2)))
        def _():
            for u in units(c):
                chain(u).start()

        if c % 2 == 1:
            @pl.when((t == 0) | (late & (t == 1)))
            def _():
                around(c).start()

    def step_g(c):
        mine = both(gath.at[m, c])
        for device in (right, left):
            channel(4, c, mine, mine, device).start()
        if c >= half:
            remote(mine, mine, send.at[5], recv.at[bases[4] + 1], across).start()

    def step_z2(c):
        for u in units(c):
            chain(u).wait_recv()
            for level in range(u * HOP, (u + 1) * HOP):
                za_out[level] += za_in[level]
            chain(u).start()

    def step_z3(c):
        if c % 2 == 1:
            around(c).wait_recv()
            relay(c).start()

    def step_d():
        arrive(4, 0, near.at[pl.ds(0, half)])
        for c in range(half):
            channel(5, 0, gath.at[mem_l, c, 0], gath.at[mem_l, c, 0], right).start()
            channel(5, 0, gath.at[mem_r, c, 1], gath.at[mem_r, c, 1], left).start()

    def early_1(level):
        return za_in[level]

    def early_23(level):
        return za_in[level] + zb_in[level]

    def step_e(c, early):
        def come():
            for u in units(c):
                chain(u).wait_recv()

        if early is early_23 and c % 2 == 0:
            @pl.when(t == 2)
            def _():
                relay(c + 1).wait_recv()

            @pl.when(late & (t == 3))
            def _():
                bypass(c + 1).wait_recv()

        pl.when((t != 2) | late)(come)
        for level in range(lc):
            gath[m, c, 2, level] = early(c * lc + level)
        if early is early_23:
            @pl.when(late & (t == 3))
            def _():
                for level in range(lc):
                    gath[m, c, 2, level] += zc_in[c * lc + level]

        for device in (across, right, left):
            channel(6, c, gath.at[m, c, 2], gath.at[m, c, 2], device).start()

    def play(steps):
        for step, *args in steps:
            with scope(f"{step.__name__.replace("step_","").upper()[0]}{args[0]}"):
                step(*args)

    every = range(nc)
    first = [(step_a, c) for c in ringed[:1]]
    for k in range(max(DIRECT, nc - DIRECT - 1)):
        if k < DIRECT:
            first.append((step_b, k))
        if DIRECT + 1 + k < nc:
            first.append((step_a, DIRECT + 1 + k))
    play(first)

    def rest(also=None):
        for c in ringed:
            play([(step_b, c)])
            if also is not None:
                play([(also, c)])
            play([(step_g, k) for k in (range(DIRECT + 1) if c == DIRECT else (c,))])

    @pl.when(t == 0)
    def _():
        rest()
        step_d()

        @pl.when(late)
        def _():
            for c in range(1, nc, 2):
                around(c).wait_recv()
                bypass(c).start()

    @pl.when(t == 1)
    def _():
        play([(step_b, c) for c in ringed] + [(step_g, c) for c in every])
        play([(step_e, c, early_1) for c in range(half)])
        step_d()
        play([(step_e, c, early_1) for c in range(half, nc)])

    @pl.when((t == 2) & jnp.logical_not(late))
    def _():
        play([(step_z2, c) for c in direct])
        rest(step_z2)

    @pl.when((t == 2) & late)
    def _():
        rest()

    @pl.when(t == 2)
    def _():
        play([(step_e, c, early_23) for c in range(half)])
        step_d()
        play([(step_e, c, early_23) for c in range(half, nc)])

    @pl.when(t == 3)
    def _():
        play([(step_z3, c) for c in direct])
        rest(step_z3)
        step_d()
        play([(step_e, c, early_23) for c in every])

    with scope("P"):
        arrive(4, half, mail.at[pl.ds(0, half)])
        arrive(5, 0, far.at[pl.ds(0, half)])
    with scope("H"):
        @pl.when(t > 0)
        def _():
            arrive(6, 0, gath.at[0])

    with scope("W"):
        @pl.when(sends_r)
        def _():
            to_right(right_tile).wait_send()

        @pl.when(sends_l)
        def _():
            to_left(last_tile).wait_send()

        @pl.when((low & tail) | (odd & head))
        def _():
            wrap_r.wait_send()

        sent(0, far)
        sent(1, near)
        sent(4, near)
        sent(5, far)

        @pl.when(t < 3)
        def _():
            sent(2, za_out)

        @pl.when((t == 0) | (t == 3))
        def _():
            sent(3, za_out)

        @pl.when(late & (t == 1))
        def _():
            sent(3, za_out)

        @pl.when(late & (t == 0))
        def _():
            sent(7, za_out)

        @pl.when(t > 0)
        def _():
            sent(6, gath.at[0])


def blend_kernel(gath, scale, out, block, sems):
    n_mem, nc, _, lc = gath.shape[:4]
    windows = block.shape[0]
    copies = []
    for w in range(windows):
        a, b = scale[w, 0], scale[w, 1]
        for q in range(n_mem):
            for c in range(nc):
                for level in range(lc):
                    r0, r1, e = (gath[q, c, i, level] for i in range(3))
                    block[w, (q * nc + c) * lc + level] = e + (a * r0 + b * r1)
        copies.append(pltpu.make_async_copy(block.at[w], out.at[w], sems.at[w]))
        copies[-1].start()
    for copy in copies:
        copy.wait()


def solution(mesh):
    n_tm, n_mem, n_tile = (mesh.shape[a] for a in ("tm", "mem", "tile"))

    def folded(x):
        *lead, rows, columns = x.shape
        x = x.reshape(*lead, rows, columns // 128, 128)
        x = jnp.swapaxes(x, -3, -2)
        return x.reshape(*lead, rows * (columns // 128), 128)

    def per_device(control, vertical_modes, mode_counts, perturbations, slot_index, blend_weight):
        members, slots, levels = perturbations.shape[:3]
        windows = slot_index.shape[0]
        ctrl = folded(control).reshape(-1, 128)
        pert = folded(perturbations).reshape(members, slots, levels // 2, 16, 128)
        rows = ctrl.shape[0]
        nc = CHUNKS
        lc = levels // n_mem // nc
        f32 = jnp.float32
        slot = (nc, slots, lc, 8, 128)
        one = (nc * lc, 8, 128)
        vmem = pl.BlockSpec(memory_space=pltpu.VMEM)
        hbm = pl.BlockSpec(memory_space=pl.ANY)
        dma = pltpu.SemaphoreType.DMA
        regular = pltpu.SemaphoreType.REGULAR
        gath, scale = pl.pallas_call(
            functools.partial(kernel, n_tm, n_mem, n_tile, members, windows),
            out_shape=(
                pltpu.VMEM((n_mem, nc, 3, lc, 8, 128), f32),
                pltpu.VMEM((windows, 2, 8, 128), f32),
            ),
            in_specs=[hbm] * 6,
            out_specs=(vmem, vmem),
            scratch_shapes=[
                pltpu.VMEM((3, rows, 128), f32), pltpu.VMEM((8 * -(-2 * members // 8), 8, 128), f32),
                pltpu.VMEM(pert.shape, jnp.bfloat16),
                pltpu.VMEM((rows, 128), f32),
                pltpu.VMEM(slot, f32), pltpu.VMEM((nc, 2, *slot[1:]), f32),
                pltpu.VMEM(slot, f32), pltpu.VMEM((nc, 3, *slot[1:]), f32),
                pltpu.VMEM(one, f32), pltpu.VMEM(one, f32), pltpu.VMEM(one, f32), pltpu.VMEM(one, f32),
                pltpu.SMEM((2, levels), f32), pltpu.SMEM(mode_counts.shape, jnp.int32),
                pltpu.SMEM((windows,), jnp.int32), pltpu.SMEM((windows,), f32),
                dma((5,)), dma((8,)), dma((2 * nc - DIRECT + nc * lc // HOP + nc + 4,)), regular, regular,
            ],
            compiler_params=pltpu.CompilerParams(collective_id=0, has_side_effects=True),
        )(ctrl, pert, vertical_modes.T, mode_counts, slot_index, blend_weight)
        out = pl.pallas_call(
            blend_kernel,
            out_shape=jax.ShapeDtypeStruct((windows, levels, 8, 128), f32),
            in_specs=[vmem, vmem],
            out_specs=hbm,
            scratch_shapes=[pltpu.VMEM((windows, levels, 8, 128), f32), dma((windows,))],
        )(*(pltpu.with_memory_space_constraint(x, pltpu.VMEM) for x in (gath, scale)))
        out = out.reshape(windows, levels, 2, 4, 128)
        return jnp.swapaxes(out, -3, -2).reshape(windows, levels, 4, 256)

    return jax.shard_map(
        per_device,
        mesh=mesh,
        in_specs=(
            P("mem", None, "tile", None), P(), P("tile"),
            P("mem", "tm", None, "tile", None), P("tm"), P("tm"),
        ),
        out_specs=P("tm", None, "tile", None),
        check_vma=False,
    )
```
